32 devices in a mesh: gx: 4 (over x, core), gy: 4 (over z), gz: 2 (over y).
Axes of the slice: x: 2, y: 2, z: 4, core: 2. Of those that a mesh axis runs over, the one named last changes fastest.
Arguments:
- columns: int32 [1024, 2048], P(('gx', 'gy', 'gz')), may hold values from 0 to 32767, as said below
- counts: int32 [1024, 2048], P(('gx', 'gy', 'gz')), may hold values from 1 to 63
- nnz_count: int32 [1024], P(('gx', 'gy', 'gz')), may hold values from 1 to 2048, as said below
- selected: int32 [2048], replicated, may hold values from 0 to 32767, as said below
Outputs:
- gene_stats: float32 [2, 32768], P(None, 'gz')
- pca_input: bfloat16 [1024, 2048], P(('gx', 'gy'), 'gz')
The draws below stay inside these ranges and needn't reach their ends.
Inputs may be any that keep to these rules, and one draw needn't show every extreme that they name: `columns`: in each row no two slots fall in the same block of 16 consecutive genes (so the first nnz_count slots hold distinct genes); slots beyond nnz_count are not part of the matrix. For every k, the live slots of one cell fall on at most 128 of the genes selected[k * 2048 / 2] to selected[(k + 1) * 2048 / 2 - 1]; some cell reaches 128 for every k in every draw. `nnz_count`: some cell has all 2048 slots live in every draw. `selected`: distinct genes.
All inputs are finite; a program needn't handle non-finite values.
Results may differ from the reference program's by a relative error of at most 0.0085.
Values may be sent and summed in bfloat16 or wider, within the bound.
A program may use at most 128 MiB of HBM per device.

```python
import jax
import jax.numpy as jnp
from jax import lax

GENES = 32768
SEL = 2048
NNZ_MAX = 2048
CELLS = 1024
N_GZ = 2


def block_plan(key):
    stride = GENES // NNZ_MAX
    share_size = SEL // N_GZ
    per_owner = 2 * share_size // stride
    block_order = jax.random.permutation(jax.random.fold_in(key, 31), jnp.arange(NNZ_MAX, dtype=jnp.int32))[:N_GZ * per_owner]
    block_order = block_order.reshape(N_GZ, per_owner).astype(jnp.int32)
    block_keys = jax.random.split(jax.random.fold_in(key, 32), N_GZ * per_owner)
    lane_perm = jax.vmap(lambda one_key: jax.random.permutation(one_key, jnp.arange(stride, dtype=jnp.int32)))(block_keys)
    return (block_order, lane_perm.reshape(N_GZ, per_owner, stride).astype(jnp.int32))


def full_cell(key):
    return jax.random.randint(jax.random.fold_in(key, 41), (), 0, CELLS, dtype=jnp.int32)


def draw_columns(key, part):
    stride = GENES // NNZ_MAX
    block_order, lane_perm = block_plan(key)
    forced = jnp.full((NNZ_MAX,), -1, jnp.int32).at[block_order.reshape(-1)].set(lane_perm[:, :, 0].reshape(-1))
    jitter = jax.random.randint(jax.random.fold_in(key, 12), (CELLS, NNZ_MAX), 0, stride, dtype=jnp.int32)
    cell_ids = lax.broadcasted_iota(jnp.int32, (CELLS, NNZ_MAX), 0)
    pinned = (cell_ids == full_cell(key)) & (forced[None, :] >= 0)
    jitter = jnp.where(pinned, forced[None, :], jitter)
    block_ids = lax.broadcasted_iota(jnp.int32, (CELLS, NNZ_MAX), 1)
    genes_drawn = block_ids * stride + jitter
    shuffled = jax.random.permutation(jax.random.fold_in(key, 14), genes_drawn, axis=1, independent=True)
    return shuffled.astype(jnp.int32)


def draw_nnz_count(key, part):
    cell_ids = jnp.arange(CELLS, dtype=jnp.int32)
    lowest = NNZ_MAX // 3
    base = lowest + (NNZ_MAX - lowest) * cell_ids // max(CELLS - 1, 1)
    floor_count = jnp.maximum(base // 2, 1)
    spread = base - floor_count + 1
    draw_bits = jax.random.randint(jax.random.fold_in(key, 21), (CELLS,), 0, 1 << 20, dtype=jnp.int32)
    picked = floor_count + draw_bits * spread // (1 << 20)
    picked = jnp.where(cell_ids == full_cell(key), NNZ_MAX, picked)
    return jnp.clip(picked, 1, NNZ_MAX).astype(jnp.int32)


def draw_selected(key, part):
    stride = GENES // NNZ_MAX
    share_size = SEL // N_GZ
    per_owner = 2 * share_size // stride
    block_order, lane_perm = block_plan(key)
    gene_grid = block_order[:, :, None] * stride + lane_perm
    anchors = gene_grid[:, :, 0]
    others = gene_grid[:, :, 1:].reshape(N_GZ, per_owner * (stride - 1))
    other_keys = jax.random.split(jax.random.fold_in(key, 33), N_GZ)
    others = jax.vmap(lambda one_key, row_genes: jax.random.permutation(one_key, row_genes))(other_keys, others)
    others = others[:, :share_size - per_owner]
    chosen = jnp.concatenate([anchors, others], axis=1)
    order_keys = jax.random.split(jax.random.fold_in(key, 34), N_GZ)
    chosen = jax.vmap(lambda one_key, row_genes: jax.random.permutation(one_key, row_genes))(order_keys, chosen)
    return chosen.reshape(-1).astype(jnp.int32)


def with_ends(drawn, key, low, top_value):
    longest = drawn.shape.index(max(drawn.shape))
    spots = []
    for shift in (0, 1):
        where = [jax.random.randint(jax.random.fold_in(key, axis), (), 0, length) for axis, length in enumerate(drawn.shape)]
        where[longest] = (where[longest] + shift) % drawn.shape[longest]
        spots.append(tuple(where))
    return drawn.at[spots[0]].set(low).at[spots[1]].set(top_value)


def setup_inputs(seed: int = 0) -> dict:
    streams_of = jax.random.split(jax.random.key(seed), 5)
    return {
        "columns": draw_columns(jax.random.fold_in(streams_of[4], 71), 0),
        "counts": with_ends(jax.random.randint(streams_of[1], (CELLS, NNZ_MAX), 1, 64), jax.random.fold_in(streams_of[1], 1), 1, 63).astype(jnp.int32),
        "nnz_count": draw_nnz_count(jax.random.fold_in(streams_of[4], 71), 0),
        "selected": draw_selected(jax.random.fold_in(streams_of[4], 71), 0),
    }


target_sum = 10000.0
var_floor = 0.01
clip_value = 10.0

def reference(columns, counts, nnz_count, selected):
    slot = lax.broadcasted_iota(jnp.int32, counts.shape, 1)
    live = slot < nnz_count[:, None]
    raw = jnp.where(live, counts.astype(jnp.float32), jnp.float32(0.0))
    library = lax.optimization_barrier(jnp.sum(raw, axis=1, keepdims=True))
    values = jnp.log1p(raw * (target_sum / library))
    genes = jnp.where(live, columns, 0).astype(jnp.int32).reshape(-1)
    flat = values.reshape(-1)
    total = jax.ops.segment_sum(flat, genes, num_segments=GENES)
    square = jax.ops.segment_sum(flat * flat, genes, num_segments=GENES)
    mean = total / CELLS
    variance = square / CELLS - mean * mean
    gene_stats = jnp.stack([mean, variance])
    table = jnp.full((GENES,), SEL, jnp.int32).at[selected].set(jnp.arange(SEL, dtype=jnp.int32))
    position = table[genes]
    rows = jnp.repeat(jnp.arange(CELLS, dtype=jnp.int32), NNZ_MAX)
    index = rows * (SEL + 1) + position
    dense = jax.ops.segment_sum(flat, index, num_segments=CELLS * (SEL + 1)).reshape(CELLS, SEL + 1)[:, :SEL]
    mean_sel = mean[selected]
    scale_sel = jnp.sqrt(jnp.maximum(variance[selected], var_floor))
    pca_input = jnp.clip((dense - mean_sel[None, :]) / scale_sel[None, :], -clip_value, clip_value).astype(jnp.bfloat16)
    return (gene_stats, pca_input)
```

```python
import functools

import jax
import jax.numpy as jnp
from jax import lax
from jax.experimental import pallas as pl
from jax.experimental.pallas import tpu as pltpu
from jax.sharding import PartitionSpec as P

GENES = 32768
BLOCK = 16
LANES = 128
GROUP = 8
HIGHS = GENES // (BLOCK * LANES)

target_sum = 10000.0
var_floor = 0.01
clip_value = 10.0

MESH = pl.DeviceIdType.MESH


def flip(value, k, size):
    out, bit = 0, 1
    while bit < size:
        part = lax.rem(lax.div(value, bit), 2)
        out = out + (1 - part if k & bit else part) * bit
        bit *= 2
    return out


def fused_kernel(
    sizes, cells, columns_hbm, counts_hbm, nnz_hbm, selected_hbm, gene_ref, pca_ref,
    columns_ref, counts_ref, nnz_ref, selected_ref, value_rows, high_rows, low_rows, offset_rows,
    near_values, near_squares, near_offsets, far_values, far_offsets, acc_values, acc_squares, table,
    sums_ref, sel_sums_ref, dense_ref, got, sel_got, mine, sel_mine, stats_ref, sel_stats_ref, moved_ref,
    wide, turned, load_sem, send_sem, recv_sem,
):
    nx, ny, owners = sizes
    teams = nx * ny
    n = teams * owners
    gx, gy, z = lax.axis_index("gx"), lax.axis_index("gy"), lax.axis_index("gz")
    r = gx * ny + gy
    me = r * owners + z
    bf16, f32 = jnp.bfloat16, jnp.float32
    local, slots = columns_ref.shape
    groups = local // GROUP
    tiles = slots // LANES
    rows = HIGHS // owners

    loads = [pltpu.make_async_copy(nnz_hbm, nnz_ref, load_sem.at[0])]
    for g in range(groups):
        span = pl.ds(g * GROUP, GROUP)
        loads.append(pltpu.make_async_copy(counts_hbm.at[span], counts_ref.at[span], load_sem.at[1 + 2 * g]))
        loads.append(pltpu.make_async_copy(columns_hbm.at[span], columns_ref.at[span], load_sem.at[2 + 2 * g]))
    loads.append(pltpu.make_async_copy(selected_hbm, selected_ref, load_sem.at[1 + 2 * groups]))
    for load in loads:
        load.start()

    small = n <= 64
    if small:
        xs = [flip(gx, k, nx) for k in range(nx)]
        ys = [flip(gy, k, ny) for k in range(ny)]
        zs = [flip(z, k, owners) for k in range(owners)]
        steps = [(kx, ky, kz) for ky in range(ny) for kx in range(nx) for kz in range(owners)]
        steps = [step for step in reversed(steps) if any(step)]

    def each_device(act):
        if small:
            for kx, ky, kz in steps:
                other = (xs[kx] * ny + ys[ky]) * owners + zs[kz]
                act(other, {"gx": xs[kx], "gy": ys[ky], "gz": zs[kz]})
            return

        def step(k, carry):
            other = lax.rem(me + k, n)
            team, owner = lax.div(other, owners), lax.rem(other, owners)
            act(other, {"gx": lax.div(team, ny), "gy": lax.rem(team, ny), "gz": owner})
            return carry

        lax.fori_loop(1, n, step, 0)

    def each_team(act):
        if small:
            for kx, ky, kz in steps:
                if kz == 0:
                    act({"gx": xs[kx], "gy": ys[ky], "gz": z})
            return

        def step(k, carry):
            team = lax.rem(r + k, teams)
            act({"gx": lax.div(team, ny), "gy": lax.rem(team, ny), "gz": z})
            return carry

        lax.fori_loop(1, teams, step, 0)

    barrier = pltpu.get_barrier_semaphore()
    each_device(
        lambda other, where: pl.semaphore_signal(barrier, inc=1, device_id=where, device_id_type=MESH)
    )

    def send(src, dst, kind, where):
        pltpu.make_async_remote_copy(
            src_ref=src, dst_ref=dst, send_sem=send_sem.at[kind], recv_sem=recv_sem.at[kind],
            device_id=where, device_id_type=MESH,
        ).start()

    def finish(sem, ref, count):
        span = ref.at[pl.ds(0, count)]
        pltpu.make_async_copy(span, span, sem).wait()

    ids = lax.broadcasted_iota(jnp.int32, (16, slots), 0).astype(f32).astype(bf16)
    sub = lax.broadcasted_iota(jnp.int32, (GROUP, local), 0)
    lane = lax.broadcasted_iota(jnp.int32, (GROUP, local), 1)
    slot = lax.broadcasted_iota(jnp.int32, (GROUP, slots), 1)

    def prepare(g):
        loads[1 + 2 * g].wait()
        span = slice(g * GROUP, (g + 1) * GROUP)
        live_count = jnp.sum(jnp.where(sub + g * GROUP == lane, nnz_ref[...], 0), axis=1, keepdims=True)
        live = slot < live_count
        raw = jnp.where(live, counts_ref[span, :].astype(f32), 0.0)
        library = jnp.sum(raw, axis=1, keepdims=True)
        value = jnp.log(1.0 + raw * (target_sum / library))
        loads[2 + 2 * g].wait()
        genes = columns_ref[span, :]
        upper = (lax.shift_right_logical(genes, 10) & 1) * HIGHS
        high = (lax.shift_right_logical(genes, 11) + upper).astype(f32)
        low = (lax.shift_right_logical(genes, 4) & (LANES // 2 - 1)).astype(f32)
        offset = jnp.where(live, genes & (BLOCK - 1), 0).astype(f32)
        for tile in range(tiles):
            at = (g * tiles + tile) * GROUP
            cols = slice(tile * LANES, (tile + 1) * LANES)
            for ref, line in ((value_rows, value), (high_rows, high), (low_rows, low), (offset_rows, offset)):
                ref[at:at + GROUP, :] = line[:, cols]

    def spread(ref, g, j):
        return jnp.concatenate(
            [ref[pl.ds((g * tiles + tile) * GROUP + j, 16, stride=0), :].astype(bf16) for tile in range(tiles)],
            axis=1,
        )

    def place(g, j):
        c = g * GROUP + j
        zero, one = bf16(0.0), bf16(1.0)
        high = spread(high_rows, g, j)
        hits = [high == ids + bf16(HIGHS * k) for k in range(2)]
        value, offset = spread(value_rows, g, j), spread(offset_rows, g, j)
        left = jnp.concatenate(
            [jnp.where(hit, line, zero) for line in (value, offset) for hit in hits], axis=0
        )
        low = spread(low_rows, g, j)
        right = jnp.concatenate(
            [jnp.where(low == ids + bf16(16 * k), one, zero) for k in range(LANES // 32)], axis=0
        )
        placed = lax.dot_general(left, right, (((1,), (1,)), ((), ())), preferred_element_type=f32)
        quarters = [placed[HIGHS * k:HIGHS * (k + 1)] for k in range(4)]
        v = jnp.concatenate(quarters[:2], axis=1)
        o = jnp.concatenate(quarters[2:], axis=1)
        near_values[c], near_squares[c], near_offsets[c] = v, v * v, o
        far_values[pl.ds(c, HIGHS, stride=local), :] = v
        far_offsets[pl.ds(c, HIGHS, stride=local), :] = o

    def gather_sums(g, ks):
        total = [jnp.zeros((HIGHS, LANES), f32) if g == 0 else acc_values[k] for k in ks]
        square = [jnp.zeros((HIGHS, LANES), f32) if g == 0 else acc_squares[k] for k in ks]
        for j in range(GROUP):
            c = g * GROUP + j
            v, w, o = near_values[c], near_squares[c], near_offsets[c]
            for i, k in enumerate(ks):
                hit = o == float(k)
                total[i] = total[i] + jnp.where(hit, v, 0.0)
                square[i] = square[i] + jnp.where(hit, w, 0.0)
        for i, k in enumerate(ks):
            if g < groups - 1:
                acc_values[k], acc_squares[k] = total[i], square[i]
                continue
            near = total[i] * (1.0 / local)
            spare = square[i] - total[i] * near
            for owner in range(owners):
                part = slice(owner * rows, (owner + 1) * rows)
                sums_ref[k * owners + owner] = jnp.concatenate([near[part], spare[part]], axis=0).astype(bf16)

    per_cell = BLOCK // GROUP
    loads[0].wait()
    for g in range(groups):
        with jax.named_scope("prep"):
            prepare(g)
        with jax.named_scope("place"):
            for j in range(GROUP):
                place(g, j)
                if g:
                    gather_sums(g - 1, range(j * per_cell, (j + 1) * per_cell))
    with jax.named_scope("tail"):
        for j in range(GROUP):
            gather_sums(groups - 1, range(j * per_cell, (j + 1) * per_cell))

    with jax.named_scope("barrier_wait"):
        pl.semaphore_wait(barrier, n - 1)
    with jax.named_scope("scatter_send"):
        each_device(lambda other, where: send(sums_ref.at[other], got.at[me], 0, where))
    got[me] = sums_ref[me]

    with jax.named_scope("select"):
        share = dense_ref.shape[2]
        out_tiles = share // LANES
        chunk = min(256, share)
        pairs = HIGHS // 2
        for pair in range(pairs):
            for part, ref in enumerate((far_values, far_offsets)):
                at = 2 * pair * local
                line = jnp.concatenate([ref[at:at + local, :], ref[at + local:at + 2 * local, :]], axis=1)
                at = (2 * pair + part) * local
                table[at:at + local, :] = line.astype(bf16)
        sel_sums_ref[...] = jnp.zeros_like(sel_sums_ref)
        chunk_ids = lax.broadcasted_iota(jnp.int32, (16, chunk), 0).astype(f32).astype(bf16)
        loads[1 + 2 * groups].wait()
        for first in range(0, owners * share, chunk):
            picked = selected_ref[:, first:first + chunk]
            inside = (lax.shift_right_logical(picked, 4) & (2 * LANES - 1)).astype(f32)
            inside = jnp.broadcast_to(inside, (16, chunk)).astype(bf16)
            one_hot = jnp.concatenate(
                [jnp.where(inside == chunk_ids + bf16(16 * k), bf16(1.0), bf16(0.0)) for k in range(16)], axis=0
            )
            found = jnp.dot(table[...], one_hot, preferred_element_type=f32)
            which = jnp.broadcast_to(lax.shift_right_logical(picked, 12), (2 * local, chunk))
            mix = found[:2 * local]
            for pair in range(1, pairs):
                mix = jnp.where(which == pair, found[2 * local * pair:2 * local * (pair + 1)], mix)
            wanted = (picked & (BLOCK - 1)).astype(f32)
            x = jnp.where(mix[local:] == wanted, mix[:local], 0.0)
            owner, start = first // share, first % share
            dense_ref[owner, :, start:start + chunk] = x.astype(bf16)
            total = jnp.sum(x, axis=0, keepdims=True)
            square = jnp.sum(x * x, axis=0, keepdims=True)
            for stat, line in enumerate((total, square)):
                for tile in range(chunk // LANES):
                    line_row = stat * out_tiles + start // LANES + tile
                    sel_sums_ref[line_row * owners + owner] = line[:, tile * LANES:(tile + 1) * LANES]

    with jax.named_scope("sel_send"):
        each_device(lambda other, where: send(sel_sums_ref.at[other], sel_got.at[me], 1, where))

        def move(k, carry):
            owner = lax.rem(z + k, owners)
            send(dense_ref.at[owner], moved_ref.at[z], 2, {"gx": gx, "gy": gy, "gz": owner})
            return carry

        lax.fori_loop(1, owners, move, 0)
        sel_got[me] = sel_sums_ref[me]
        moved_ref[z] = dense_ref[z]

    with jax.named_scope("wait_rs"):
        finish(recv_sem.at[0], got, n - 1)
    with jax.named_scope("reduce"):
        parts = got[...].astype(f32)
        means = parts[:, :rows]
        mean = jnp.sum(means, axis=0) * (1.0 / n)
        away = means - mean[None]
        variance = jnp.sum(parts[:, rows:] + (away * away) * float(local), axis=0) * (1.0 / cells)
        mine[...] = jnp.concatenate([mean, variance], axis=0).astype(bf16)
    with jax.named_scope("gather_send"):
        each_team(lambda where: send(mine, stats_ref.at[r], 3, where))
    with jax.named_scope("wait_selrs"):
        finish(recv_sem.at[1], sel_got, n - 1)
    with jax.named_scope("selreduce"):
        sel_mine[...] = jnp.sum(sel_got[...], axis=0)
        each_team(lambda where: send(sel_mine, sel_stats_ref.at[r], 4, where))
        stats_ref[r] = mine[...]
        sel_stats_ref[r] = sel_mine[...]
    with jax.named_scope("wait_moved"):
        finish(recv_sem.at[2], moved_ref, owners - 1)
        finish(send_sem.at[0], got, n - 1)
        finish(send_sem.at[1], sel_got, n - 1)
        finish(send_sem.at[2], moved_ref, owners - 1)
    with jax.named_scope("wait_stats"):
        finish(recv_sem.at[3], stats_ref, teams - 1)
    with jax.named_scope("genes"):
        wide[...] = stats_ref[...].astype(f32).reshape(wide.shape)
        lines = rows * LANES // BLOCK * 2
        for stat in range(2):
            for row in range(rows):
                line = wide[pl.ds(stat * rows + row, teams, stride=2 * rows), :]
                turned[row * LANES:(row + 1) * LANES, :] = jnp.transpose(line)
            parts = [turned[pl.ds(k, lines, stride=8), :] for k in range(8)]
            gene_ref[:, stat, :] = jnp.concatenate(parts, axis=1)
    with jax.named_scope("wait_sel"):
        finish(recv_sem.at[4], sel_stats_ref, teams - 1)
    with jax.named_scope("pca"):
        for tile in range(out_tiles):
            mean = sel_stats_ref[tile] * (1.0 / cells)
            variance = sel_stats_ref[out_tiles + tile] * (1.0 / cells) - mean * mean
            scale = 1.0 / jnp.sqrt(jnp.maximum(variance, var_floor))
            cols = slice(tile * LANES, (tile + 1) * LANES)
            for owner in range(owners):
                x = moved_ref[owner, :, cols].astype(f32)
                y = jnp.clip((x - mean) * scale, -clip_value, clip_value)
                pca_ref[owner * local:(owner + 1) * local, cols] = y.astype(bf16)
    with jax.named_scope("wait_sends"):
        finish(send_sem.at[3], stats_ref, teams - 1)
        finish(send_sem.at[4], sel_stats_ref, teams - 1)


def per_device(sizes, columns, counts, nnz_count, selected):
    f32, bf16, i32 = jnp.float32, jnp.bfloat16, jnp.int32
    nx, ny, owners = sizes
    teams = nx * ny
    n = teams * owners
    local, slots = columns.shape
    rows = HIGHS // owners
    share = selected.shape[0] // owners
    assert teams == BLOCK and rows * owners == HIGHS and rows <= 8 and 2 * share // LANES <= teams
    assert local % GROUP == 0
    hbm = pl.BlockSpec(memory_space=pltpu.HBM)
    vmem = pl.BlockSpec(memory_space=pltpu.VMEM)
    lines = GENES // owners // LANES
    slot_rows = local * slots // LANES + 16
    far_rows = HIGHS * local
    arrays = (columns, counts, nnz_count.reshape(1, local), selected.reshape(1, -1))
    gene_stats, pca_input = pl.pallas_call(
        functools.partial(fused_kernel, sizes, local * n),
        name="moments_and_selection",
        out_shape=(pltpu.VMEM((lines, 2, LANES), f32), pltpu.VMEM((owners * local, share), bf16)),
        in_specs=[hbm] * 4,
        out_specs=(vmem,) * 2,
        scratch_shapes=[
            pltpu.VMEM((local, slots), i32),
            pltpu.VMEM((local, slots), i32),
            pltpu.VMEM((1, local), i32),
            pltpu.VMEM((1, owners * share), i32),
        ]
        + [pltpu.VMEM((slot_rows, LANES), f32)] * 4
        + [pltpu.VMEM((local, HIGHS, LANES), f32)] * 3
        + [pltpu.VMEM((far_rows, LANES), f32)] * 2
        + [pltpu.VMEM((BLOCK, HIGHS, LANES), f32)] * 2
        + [
            pltpu.VMEM((far_rows, 2 * LANES), bf16),
            pltpu.VMEM((n, 2 * rows, LANES), bf16),
            pltpu.VMEM((n, 1, LANES), f32),
            pltpu.VMEM((owners, local, share), bf16),
            pltpu.VMEM((n, 2 * rows, LANES), bf16),
            pltpu.VMEM((n, 1, LANES), f32),
            pltpu.VMEM((2 * rows, LANES), bf16),
            pltpu.VMEM((1, LANES), f32),
            pltpu.VMEM((teams, 2 * rows, LANES), bf16),
            pltpu.VMEM((teams, 1, LANES), f32),
            pltpu.VMEM((owners, local, share), bf16),
            pltpu.VMEM((teams * 2 * rows, LANES), f32),
            pltpu.VMEM((rows * LANES, teams), f32),
            pltpu.SemaphoreType.DMA((2 + 2 * (local // GROUP),)),
            pltpu.SemaphoreType.DMA((5,)),
            pltpu.SemaphoreType.DMA((5,)),
        ],
        compiler_params=pltpu.CompilerParams(
            collective_id=0, has_side_effects=True, vmem_limit_bytes=32 * 1024 * 1024
        ),
    )(*(pltpu.with_memory_space_constraint(array, pltpu.HBM) for array in arrays))
    return (gene_stats.transpose(1, 0, 2).reshape(2, -1), pca_input)


def solution(mesh):
    sizes = tuple(mesh.shape[axis] for axis in ("gx", "gy", "gz"))
    return jax.shard_map(
        functools.partial(per_device, sizes),
        mesh=mesh,
        in_specs=(
            P(("gx", "gy", "gz"), None),
            P(("gx", "gy", "gz"), None),
            P(("gx", "gy", "gz")),
            P(),
        ),
        out_specs=(P(None, "gz"), P(("gx", "gy"), "gz")),
        check_vma=False,
    )
```

```python
import functools

import jax
import jax.numpy as jnp
from jax import lax
from jax.experimental import pallas as pl
from jax.experimental.pallas import tpu as pltpu
from jax.sharding import PartitionSpec as P

GENES = 32768
BLOCK = 16
LANES = 128
GROUP = 8
HIGHS = GENES // (BLOCK * LANES)
WIDTH = 8
BASE = 60
QUARTERS = 4

target_sum = 10000.0
var_floor = 0.01
clip_value = 10.0

MESH = pl.DeviceIdType.MESH


def flip(value, k, size):
    out, bit = 0, 1
    while bit < size:
        part = lax.rem(lax.div(value, bit), 2)
        out = out + (1 - part if k & bit else part) * bit
        bit *= 2
    return out


def fused_kernel(
    sizes, cells, columns_hbm, counts_hbm, nnz_hbm, selected_hbm, stats_ref, sel_stats_ref, moved_ref,
    columns_ref, counts_ref, nnz_ref, selected_ref, code_rows, high_rows, low_rows,
    near_values, near_squares, near_offsets, far_codes, acc_values, acc_squares, table,
    mean_rows, spare_rows, sums_ref, sel_sums_ref, dense_ref, got, sel_got, mine, sel_mine, turned,
    load_sem, send_sem, recv_sem,
):
    nx, ny, owners = sizes
    teams = nx * ny
    n = teams * owners
    gx, gy, z = lax.axis_index("gx"), lax.axis_index("gy"), lax.axis_index("gz")
    r = gx * ny + gy
    me = r * owners + z
    bf16, f32 = jnp.bfloat16, jnp.float32
    local, slots = columns_ref.shape
    groups = local // GROUP
    tiles = slots // LANES
    span_blocks = GENES // (BLOCK * n)
    rows = HIGHS // owners
    halves = LANES // span_blocks
    lines = 2 * span_blocks // (LANES // BLOCK)

    loads = [pltpu.make_async_copy(nnz_hbm, nnz_ref, load_sem.at[0])]
    for g in range(groups):
        span = pl.ds(g * GROUP, GROUP)
        loads.append(pltpu.make_async_copy(counts_hbm.at[span], counts_ref.at[span], load_sem.at[1 + 2 * g]))
        loads.append(pltpu.make_async_copy(columns_hbm.at[span], columns_ref.at[span], load_sem.at[2 + 2 * g]))
    loads.append(pltpu.make_async_copy(selected_hbm, selected_ref, load_sem.at[1 + 2 * groups]))
    for load in loads:
        load.start()

    small = n <= 64
    if small:
        xs = [flip(gx, k, nx) for k in range(nx)]
        ys = [flip(gy, k, ny) for k in range(ny)]
        zs = [flip(z, k, owners) for k in range(owners)]
        steps = [(kx, ky, kz) for ky in range(ny) for kx in range(nx) for kz in range(owners)]
        steps = [step for step in reversed(steps) if any(step)]

    def each_device(act):
        if small:
            for kx, ky, kz in steps:
                other = (xs[kx] * ny + ys[ky]) * owners + zs[kz]
                act(other, {"gx": xs[kx], "gy": ys[ky], "gz": zs[kz]})
            return

        def step(k, carry):
            other = lax.rem(me + k, n)
            team, owner = lax.div(other, owners), lax.rem(other, owners)
            act(other, {"gx": lax.div(team, ny), "gy": lax.rem(team, ny), "gz": owner})
            return carry

        lax.fori_loop(1, n, step, 0)

    def each_team(act):
        if small:
            for kx, ky, kz in steps:
                if kz == 0:
                    act({"gx": xs[kx], "gy": ys[ky], "gz": z})
            return

        def step(k, carry):
            team = lax.rem(r + k, teams)
            act({"gx": lax.div(team, ny), "gy": lax.rem(team, ny), "gz": z})
            return carry

        lax.fori_loop(1, teams, step, 0)

    barrier = pltpu.get_barrier_semaphore()
    each_device(
        lambda other, where: pl.semaphore_signal(barrier, inc=1, device_id=where, device_id_type=MESH)
    )

    def send(src, dst, kind, where):
        pltpu.make_async_remote_copy(
            src_ref=src, dst_ref=dst, send_sem=send_sem.at[kind], recv_sem=recv_sem.at[kind],
            device_id=where, device_id_type=MESH,
        ).start()

    def finish(sem, ref, count):
        span = ref.at[pl.ds(0, count)]
        pltpu.make_async_copy(span, span, sem).wait()

    ids = lax.broadcasted_iota(jnp.int32, (16, slots), 0).astype(f32).astype(bf16)
    sub = lax.broadcasted_iota(jnp.int32, (GROUP, local), 0)
    lane = lax.broadcasted_iota(jnp.int32, (GROUP, local), 1)
    slot = lax.broadcasted_iota(jnp.int32, (GROUP, slots), 1)

    def wait_group(g):
        loads[1 + 2 * g].wait()
        loads[2 + 2 * g].wait()

    def prepare(g):
        span = slice(g * GROUP, (g + 1) * GROUP)
        live_count = jnp.sum(jnp.where(sub + g * GROUP == lane, nnz_ref[...], 0), axis=1, keepdims=True)
        live = slot < live_count
        raw = jnp.where(live, counts_ref[span, :].astype(f32), 0.0)
        library = jnp.sum(raw, axis=1, keepdims=True)
        value = jnp.log(1.0 + raw * (target_sum / library))
        genes = columns_ref[span, :]
        shift = ((genes & (BLOCK - 1)) * WIDTH - BASE).astype(f32)
        code = value * jnp.exp2(shift)
        quarter = lax.shift_right_logical(genes, 9) & (QUARTERS - 1)
        high = (lax.shift_right_logical(genes, 11) + quarter * HIGHS).astype(f32)
        low = (lax.shift_right_logical(genes, 4) & (LANES // QUARTERS - 1)).astype(f32)
        for tile in range(tiles):
            at = (g * tiles + tile) * GROUP
            cols = slice(tile * LANES, (tile + 1) * LANES)
            for ref, line in ((code_rows, code), (high_rows, high), (low_rows, low)):
                ref[at:at + GROUP, :] = line[:, cols]

    def spread(ref, g, j):
        return jnp.concatenate(
            [ref[pl.ds((g * tiles + tile) * GROUP + j, 16, stride=0), :].astype(bf16) for tile in range(tiles)],
            axis=1,
        )

    def place(g, j):
        c = g * GROUP + j
        zero, one = bf16(0.0), bf16(1.0)
        high, code, low = spread(high_rows, g, j), spread(code_rows, g, j), spread(low_rows, g, j)
        left = jnp.concatenate(
            [jnp.where(high == ids + bf16(HIGHS * k), code, zero) for k in range(QUARTERS)], axis=0
        )
        right = jnp.concatenate(
            [jnp.where(low == ids + bf16(16 * k), one, zero) for k in range(LANES // (16 * QUARTERS))], axis=0
        )
        placed = lax.dot_general(left, right, (((1,), (1,)), ((), ())), preferred_element_type=f32)
        code = jnp.concatenate([placed[HIGHS * k:HIGHS * (k + 1)] for k in range(QUARTERS)], axis=1)
        far_codes[pl.ds(c, HIGHS, stride=local), :] = code
        power = jnp.log2(jnp.maximum(code, 2.0 ** (-BASE - WIDTH)))
        offset = jnp.floor((power + (BASE + 0.5 * WIDTH)) * (1.0 / WIDTH))
        value = code * jnp.exp2(BASE - WIDTH * offset)
        near_values[c], near_squares[c], near_offsets[c] = value, value * value, offset

    def gather_sums(g, ks):
        total = [jnp.zeros((HIGHS, LANES), f32) if g == 0 else acc_values[k] for k in ks]
        square = [jnp.zeros((HIGHS, LANES), f32) if g == 0 else acc_squares[k] for k in ks]
        for j in range(GROUP):
            c = g * GROUP + j
            v, w, o = near_values[c], near_squares[c], near_offsets[c]
            for i, k in enumerate(ks):
                hit = o == float(k)
                total[i] = total[i] + jnp.where(hit, v, 0.0)
                square[i] = square[i] + jnp.where(hit, w, 0.0)
        for i, k in enumerate(ks):
            if g < groups - 1:
                acc_values[k], acc_squares[k] = total[i], square[i]
                continue
            near = total[i] * (1.0 / local)
            mean_rows[pl.ds(k, HIGHS, stride=BLOCK), :] = near
            spare_rows[pl.ds(k, HIGHS, stride=BLOCK), :] = square[i] - total[i] * near

    per_cell = BLOCK // GROUP
    loads[0].wait()
    wait_group(0)
    with jax.named_scope("prep"):
        prepare(0)
    for g in range(1, groups):
        wait_group(g)
    for g in range(groups):
        with jax.named_scope("place"):
            for j in range(GROUP):
                place(g, j)
                if g:
                    gather_sums(g - 1, range(j * per_cell, (j + 1) * per_cell))
                if j == 0 and g < groups - 1:
                    prepare(g + 1)
    with jax.named_scope("tail"):
        for j in range(GROUP):
            gather_sums(groups - 1, range(j * per_cell, (j + 1) * per_cell))
        for high in range(HIGHS):
            near, spare = (ref[high * BLOCK:(high + 1) * BLOCK, :] for ref in (mean_rows, spare_rows))
            for half in range(halves):
                cols = slice(half * span_blocks, (half + 1) * span_blocks)
                pair = jnp.concatenate([near[:, cols], spare[:, cols]], axis=1)
                if 2 * span_blocks < LANES:
                    pair = jnp.concatenate([pair, jnp.zeros((BLOCK, LANES - 2 * span_blocks), f32)], axis=1)
                team = (high % rows) * halves + half
                sums_ref[team * owners + high // rows] = pair.astype(bf16)

    with jax.named_scope("barrier_wait"):
        pl.semaphore_wait(barrier, n - 1)
    with jax.named_scope("scatter_send"):
        each_device(lambda other, where: send(sums_ref.at[other], got.at[me], 0, where))
    got[me] = sums_ref[me]

    with jax.named_scope("select"):
        share = dense_ref.shape[2]
        out_tiles = share // LANES
        chunk = min(256, share)
        pairs = HIGHS // 2
        for pair in range(pairs):
            at = 2 * pair * local
            line = jnp.concatenate([far_codes[at:at + local, :], far_codes[at + local:at + 2 * local, :]], axis=1)
            table[pair * local:(pair + 1) * local, :] = line.astype(bf16)
        sel_sums_ref[...] = jnp.zeros_like(sel_sums_ref)
        chunk_ids = lax.broadcasted_iota(jnp.int32, (16, chunk), 0).astype(f32).astype(bf16)
        loads[1 + 2 * groups].wait()
        for first in range(0, owners * share, chunk):
            picked = selected_ref[:, first:first + chunk]
            inside = (lax.shift_right_logical(picked, 4) & (2 * LANES - 1)).astype(f32)
            inside = jnp.broadcast_to(inside, (16, chunk)).astype(bf16)
            one_hot = jnp.concatenate(
                [jnp.where(inside == chunk_ids + bf16(16 * k), bf16(1.0), bf16(0.0)) for k in range(16)], axis=0
            )
            found = jnp.dot(table[...], one_hot, preferred_element_type=f32)
            which = jnp.broadcast_to(lax.shift_right_logical(picked, 12), (local, chunk))
            mix = found[:local]
            for pair in range(1, pairs):
                mix = jnp.where(which == pair, found[local * pair:local * (pair + 1)], mix)
            value = mix * jnp.exp2((BASE - (picked & (BLOCK - 1)) * WIDTH).astype(f32))
            x = jnp.where((value > 2.0 ** -4.5) & (value < 2.0 ** 3.5), value, 0.0)
            owner, start = first // share, first % share
            dense_ref[owner, :, start:start + chunk] = x.astype(bf16)
            total = jnp.sum(x, axis=0, keepdims=True)
            square = jnp.sum(x * x, axis=0, keepdims=True)
            for stat, line in enumerate((total, square)):
                for tile in range(chunk // LANES):
                    line_row = stat * out_tiles + start // LANES + tile
                    sel_sums_ref[line_row * owners + owner] = line[:, tile * LANES:(tile + 1) * LANES]

    with jax.named_scope("sel_send"):
        each_device(lambda other, where: send(sel_sums_ref.at[other], sel_got.at[me], 1, where))

        def move(k, carry):
            owner = lax.rem(z + k, owners)
            send(dense_ref.at[owner], moved_ref.at[z], 2, {"gx": gx, "gy": gy, "gz": owner})
            return carry

        lax.fori_loop(1, owners, move, 0)
        sel_got[me] = sel_sums_ref[me]
        moved_ref[z] = dense_ref[z]

    with jax.named_scope("wait_rs"):
        finish(recv_sem.at[0], got, n - 1)
    with jax.named_scope("reduce"):
        parts = got[...].astype(f32)
        total = jnp.sum(parts, axis=0)
        mean = total * (1.0 / n)
        away = parts - mean[None]
        away = pltpu.roll(jnp.sum(away * away, axis=0), span_blocks, 1)
        variance = (total + away * float(local)) * (1.0 / cells)
        first_half = lax.broadcasted_iota(jnp.int32, (BLOCK, LANES), 1) < span_blocks
        turned[...] = jnp.transpose(jnp.where(first_half, mean, variance))
        pieces = [turned[pl.ds(k, lines, stride=LANES // BLOCK), :] for k in range(LANES // BLOCK)]
        mine[...] = jnp.concatenate(pieces, axis=1).astype(bf16)
    with jax.named_scope("gather_send"):
        each_team(lambda where: send(mine, stats_ref.at[r], 3, where))
    with jax.named_scope("wait_selrs"):
        finish(recv_sem.at[1], sel_got, n - 1)
    with jax.named_scope("selreduce"):
        sel_mine[...] = jnp.sum(sel_got[...], axis=0)
        each_team(lambda where: send(sel_mine, sel_stats_ref.at[r], 4, where))
        stats_ref[r] = mine[...]
        sel_stats_ref[r] = sel_mine[...]
    with jax.named_scope("wait_moved"):
        finish(recv_sem.at[2], moved_ref, owners - 1)
        finish(send_sem.at[0], got, n - 1)
        finish(send_sem.at[1], sel_got, n - 1)
        finish(send_sem.at[2], moved_ref, owners - 1)
    with jax.named_scope("wait_stats"):
        finish(recv_sem.at[3], stats_ref, teams - 1)
    with jax.named_scope("wait_sel"):
        finish(recv_sem.at[4], sel_stats_ref, teams - 1)
        finish(send_sem.at[3], stats_ref, teams - 1)
        finish(send_sem.at[4], sel_stats_ref, teams - 1)


def final_kernel(cells, stats_ref, sel_stats_ref, moved_ref, gene_hbm, pca_hbm, gene_ref, pca_ref, sem):
    f32, bf16 = jnp.float32, jnp.bfloat16
    teams, double, lanes = stats_ref.shape
    lines = double // 2
    stats = stats_ref[...].astype(f32)
    for team in range(teams):
        for stat in range(2):
            gene_ref[team * lines:(team + 1) * lines, stat, :] = stats[team, stat * lines:(stat + 1) * lines]
    gene_copy = pltpu.make_async_copy(gene_ref, gene_hbm, sem.at[0])
    gene_copy.start()
    owners, local, share = moved_ref.shape
    tiles = share // lanes
    for tile in range(tiles):
        mean = sel_stats_ref[tile] * (1.0 / cells)
        variance = sel_stats_ref[tiles + tile] * (1.0 / cells) - mean * mean
        scale = 1.0 / jnp.sqrt(jnp.maximum(variance, var_floor))
        cols = slice(tile * lanes, (tile + 1) * lanes)
        for owner in range(owners):
            x = moved_ref[owner, :, cols].astype(f32)
            y = jnp.clip((x - mean) * scale, -clip_value, clip_value)
            pca_ref[owner * local:(owner + 1) * local, cols] = y.astype(bf16)
    pca_copy = pltpu.make_async_copy(pca_ref, pca_hbm, sem.at[1])
    pca_copy.start()
    gene_copy.wait()
    pca_copy.wait()


def per_device(sizes, columns, counts, nnz_count, selected):
    f32, bf16, i32 = jnp.float32, jnp.bfloat16, jnp.int32
    nx, ny, owners = sizes
    teams = nx * ny
    n = teams * owners
    local, slots = columns.shape
    rows = HIGHS // owners
    share = selected.shape[0] // owners
    span_blocks = GENES // (BLOCK * n)
    double = 2 * span_blocks // (LANES // BLOCK)
    assert rows * owners == HIGHS and span_blocks * n * BLOCK == GENES and 2 * span_blocks <= LANES
    assert double % 2 == 0 and 2 * share // LANES <= teams and local % GROUP == 0
    hbm = pl.BlockSpec(memory_space=pltpu.HBM)
    vmem = pl.BlockSpec(memory_space=pltpu.VMEM)
    slot_rows = local * slots // LANES + 16
    far_rows = HIGHS * local
    arrays = (columns, counts, nnz_count.reshape(1, local), selected.reshape(1, -1))
    kept = pl.pallas_call(
        functools.partial(fused_kernel, sizes, local * n),
        name="moments_and_selection",
        out_shape=(
            pltpu.VMEM((teams, double, LANES), bf16),
            pltpu.VMEM((teams, 1, LANES), f32),
            pltpu.VMEM((owners, local, share), bf16),
        ),
        in_specs=[hbm] * 4,
        out_specs=(vmem,) * 3,
        scratch_shapes=[
            pltpu.VMEM((local, slots), i32),
            pltpu.VMEM((local, slots), i32),
            pltpu.VMEM((1, local), i32),
            pltpu.VMEM((1, owners * share), i32),
        ]
        + [pltpu.VMEM((slot_rows, LANES), f32)] * 3
        + [pltpu.VMEM((local, HIGHS, LANES), f32)] * 3
        + [pltpu.VMEM((far_rows, LANES), f32)]
        + [pltpu.VMEM((BLOCK, HIGHS, LANES), f32)] * 2
        + [pltpu.VMEM((far_rows // 2, 2 * LANES), bf16)]
        + [pltpu.VMEM((HIGHS * BLOCK, LANES), f32)] * 2
        + [
            pltpu.VMEM((n, BLOCK, LANES), bf16),
            pltpu.VMEM((n, 1, LANES), f32),
            pltpu.VMEM((owners, local, share), bf16),
            pltpu.VMEM((n, BLOCK, LANES), bf16),
            pltpu.VMEM((n, 1, LANES), f32),
            pltpu.VMEM((double, LANES), bf16),
            pltpu.VMEM((1, LANES), f32),
            pltpu.VMEM((LANES, BLOCK), f32),
            pltpu.SemaphoreType.DMA((2 + 2 * (local // GROUP),)),
            pltpu.SemaphoreType.DMA((5,)),
            pltpu.SemaphoreType.DMA((5,)),
        ],
        compiler_params=pltpu.CompilerParams(
            collective_id=0, has_side_effects=True, vmem_limit_bytes=32 * 1024 * 1024
        ),
    )(*(pltpu.with_memory_space_constraint(array, pltpu.HBM) for array in arrays))
    out_lines = GENES // owners // LANES
    gene_stats, pca_input = pl.pallas_call(
        functools.partial(final_kernel, local * n),
        name="standardize",
        out_shape=(pltpu.HBM((out_lines, 2, LANES), f32), pltpu.HBM((owners * local, share), bf16)),
        in_specs=[vmem] * 3,
        out_specs=(hbm,) * 2,
        scratch_shapes=[
            pltpu.VMEM((out_lines, 2, LANES), f32),
            pltpu.VMEM((owners * local, share), bf16),
            pltpu.SemaphoreType.DMA((2,)),
        ],
        compiler_params=pltpu.CompilerParams(vmem_limit_bytes=16 * 1024 * 1024),
    )(*(pltpu.with_memory_space_constraint(array, pltpu.VMEM) for array in kept))
    return (gene_stats.transpose(1, 0, 2).reshape(2, -1), pca_input)


def solution(mesh):
    sizes = tuple(mesh.shape[axis] for axis in ("gx", "gy", "gz"))
    return jax.shard_map(
        functools.partial(per_device, sizes),
        mesh=mesh,
        in_specs=(
            P(("gx", "gy", "gz"), None),
            P(("gx", "gy", "gz"), None),
            P(("gx", "gy", "gz")),
            P(),
        ),
        out_specs=(P(None, "gz"), P(("gx", "gy"), "gz")),
        check_vma=False,
    )
```

```python
import functools

import jax
import jax.numpy as jnp
from jax import lax
from jax.experimental import pallas as pl
from jax.experimental.pallas import tpu as pltpu
from jax.sharding import PartitionSpec as P

GENES = 32768
BLOCK = 16
LANES = 128
GROUP = 8
HIGHS = GENES // (BLOCK * LANES)
WIDTH = 8
BASE = 60
PARTS = 3
PART = -(-LANES // PARTS)

target_sum = 10000.0
var_floor = 0.01
clip_value = 10.0

MESH = pl.DeviceIdType.MESH


def flip(value, k, size):
    out, bit = 0, 1
    while bit < size:
        part = lax.rem(lax.div(value, bit), 2)
        out = out + (1 - part if k & bit else part) * bit
        bit *= 2
    return out


def hub_grid(nx, ny, count):
    across = max(1, count // ny)
    along = count // across
    return across, along, nx // across, ny // along


def fused_kernel(
    sizes, cells, columns_hbm, counts_hbm, nnz_hbm, selected_hbm, stats_ref, sel_stats_ref, moved_ref,
    columns_ref, counts_ref, nnz_ref, selected_ref, code_rows, high_rows, low_rows,
    near_values, near_offsets, far_codes, acc_values, acc_squares, table,
    mean_rows, spare_rows, sums_ref, sel_sums_ref, dense_ref, got, sel_got, mine, sel_mine, turned,
    load_sem, send_sem, recv_sem,
):
    nx, ny, owners = sizes
    teams = nx * ny
    n = teams * owners
    gx, gy, z = lax.axis_index("gx"), lax.axis_index("gy"), lax.axis_index("gz")
    r = gx * ny + gy
    me = r * owners + z
    bf16, f32 = jnp.bfloat16, jnp.float32
    local, slots = columns_ref.shape
    groups = local // GROUP
    tiles = slots // LANES
    hubs = HIGHS // owners
    across, along, step_x, step_y = hub_grid(nx, ny, hubs)
    hub_x, hub_y = lax.div(gx, step_x), lax.div(gy, step_y)
    hub = hub_x * along + hub_y
    is_hub = (gx == hub_x * step_x + step_x - 1) & (gy == hub_y * step_y + step_y - 1)
    is_leaf = jnp.logical_not(is_hub)
    lines = 2 * BLOCK

    loads = [pltpu.make_async_copy(nnz_hbm, nnz_ref, load_sem.at[0])]
    for g in range(groups):
        span = pl.ds(g * GROUP, GROUP)
        loads.append(pltpu.make_async_copy(counts_hbm.at[span], counts_ref.at[span], load_sem.at[1 + 2 * g]))
        loads.append(pltpu.make_async_copy(columns_hbm.at[span], columns_ref.at[span], load_sem.at[2 + 2 * g]))
    loads.append(pltpu.make_async_copy(selected_hbm, selected_ref, load_sem.at[1 + 2 * groups]))
    for load in loads:
        load.start()

    xs = [flip(gx, k, nx) for k in range(nx)]
    ys = [flip(gy, k, ny) for k in range(ny)]
    zs = [flip(z, k, owners) for k in range(owners)]
    hub_xs = [flip(hub_x, k, across) for k in range(across)]
    hub_ys = [flip(hub_y, k, along) for k in range(along)]

    def greet(where):
        pl.semaphore_signal(barrier, inc=1, device_id=where, device_id_type=MESH)

    def each_hub(act):
        for ky in reversed(range(along)):
            for kx in reversed(range(across)):
                for kz in reversed(range(owners)):
                    hx, hy = hub_xs[kx], hub_ys[ky]
                    slot = (hx * along + hy) * owners + zs[kz]
                    where = {"gx": hx * step_x + step_x - 1, "gy": hy * step_y + step_y - 1, "gz": zs[kz]}
                    if ky or kx or kz:
                        act(slot, where)
                    else:
                        pl.when(is_leaf)(functools.partial(act, slot, where))

    def each_team(act):
        for ky in reversed(range(ny)):
            for kx in sorted(range(nx), key=lambda k: (k & 1, k), reverse=True):
                if ky or kx:
                    act({"gx": xs[kx], "gy": ys[ky], "gz": z})

    barrier = pltpu.get_barrier_semaphore()
    if n <= 64:
        for ky in reversed(range(ny)):
            for kx in reversed(range(nx)):
                for kz in reversed(range(owners)):
                    if ky or kx or kz:
                        greet({"gx": xs[kx], "gy": ys[ky], "gz": zs[kz]})
    else:
        def greet_step(k, carry):
            other = lax.rem(me + k, n)
            team, owner = lax.div(other, owners), lax.rem(other, owners)
            greet({"gx": lax.div(team, ny), "gy": lax.rem(team, ny), "gz": owner})
            return carry

        lax.fori_loop(1, n, greet_step, 0)

    def send(src, dst, kind, where):
        pltpu.make_async_remote_copy(
            src_ref=src, dst_ref=dst, send_sem=send_sem.at[kind], recv_sem=recv_sem.at[kind],
            device_id=where, device_id_type=MESH,
        ).start()

    def finish(sem, ref, count):
        if count:
            span = ref.at[pl.ds(0, count)]
            pltpu.make_async_copy(span, span, sem).wait()

    ids = lax.broadcasted_iota(jnp.int32, (16, slots), 0).astype(f32).astype(bf16)
    sub = lax.broadcasted_iota(jnp.int32, (GROUP, local), 0)
    lane = lax.broadcasted_iota(jnp.int32, (GROUP, local), 1)
    slot = lax.broadcasted_iota(jnp.int32, (GROUP, slots), 1)

    def wait_group(g):
        loads[1 + 2 * g].wait()
        loads[2 + 2 * g].wait()

    def prepare(g):
        span = slice(g * GROUP, (g + 1) * GROUP)
        live_count = jnp.sum(jnp.where(sub + g * GROUP == lane, nnz_ref[...], 0), axis=1, keepdims=True)
        live = slot < live_count
        raw = jnp.where(live, counts_ref[span, :].astype(f32), 0.0)
        library = jnp.sum(raw, axis=1, keepdims=True)
        value = jnp.log(1.0 + raw * (target_sum / library))
        genes = columns_ref[span, :]
        shift = ((genes & (BLOCK - 1)) * WIDTH - BASE).astype(f32)
        code = value * jnp.exp2(shift)
        high = lax.shift_right_logical(genes, 11)
        low = lax.shift_right_logical(genes, 4) & (LANES - 1)
        for k in range(1, PARTS):
            past = low >= PART
            high = high + jnp.where(past, HIGHS, 0)
            low = low - jnp.where(past, PART, 0)
        high, low = high.astype(f32), low.astype(f32)
        for tile in range(tiles):
            at = (g * tiles + tile) * GROUP
            cols = slice(tile * LANES, (tile + 1) * LANES)
            for ref, line in ((code_rows, code), (high_rows, high), (low_rows, low)):
                ref[at:at + GROUP, :] = line[:, cols]

    def spread(ref, g, j):
        return jnp.concatenate(
            [ref[pl.ds((g * tiles + tile) * GROUP + j, 16, stride=0), :].astype(bf16) for tile in range(tiles)],
            axis=1,
        )

    def place(g, j):
        c = g * GROUP + j
        zero, one = bf16(0.0), bf16(1.0)
        high, code, low = spread(high_rows, g, j), spread(code_rows, g, j), spread(low_rows, g, j)
        left = jnp.concatenate(
            [jnp.where(high == ids + bf16(HIGHS * k), code, zero) for k in range(PARTS)], axis=0
        )
        right = jnp.concatenate(
            [jnp.where(low == ids + bf16(16 * k), one, zero) for k in range(-(-PART // 16))], axis=0
        )
        placed = lax.dot_general(left, right, (((1,), (1,)), ((), ())), preferred_element_type=f32)
        pieces = [
            placed[HIGHS * k:HIGHS * (k + 1), :min(PART, LANES - k * PART)] for k in range(PARTS)
        ]
        code = jnp.concatenate(pieces, axis=1)
        far_codes[pl.ds(c, HIGHS, stride=local), :] = code
        power = jnp.log2(jnp.maximum(code, 2.0 ** (-BASE - WIDTH)))
        offset = jnp.floor((power + (BASE + 0.5 * WIDTH)) * (1.0 / WIDTH))
        value = code * jnp.exp2(BASE - WIDTH * offset)
        near_values[c], near_offsets[c] = value, offset

    def gather_sums(g, ks):
        total = [jnp.zeros((HIGHS, LANES), f32) if g == 0 else acc_values[k] for k in ks]
        square = [jnp.zeros((HIGHS, LANES), f32) if g == 0 else acc_squares[k] for k in ks]
        for j in range(GROUP):
            c = g * GROUP + j
            v, o = near_values[c], near_offsets[c]
            for i, k in enumerate(ks):
                hit = jnp.where(o == float(k), v, 0.0)
                total[i] = total[i] + hit
                square[i] = square[i] + hit * hit
        for i, k in enumerate(ks):
            if g < groups - 1:
                acc_values[k], acc_squares[k] = total[i], square[i]
                continue
            near = total[i] * (1.0 / local)
            mean_rows[pl.ds(k, HIGHS, stride=BLOCK), :] = near
            spare_rows[pl.ds(k, HIGHS, stride=BLOCK), :] = square[i] - total[i] * near

    per_cell = BLOCK // GROUP
    loads[0].wait()
    wait_group(0)
    with jax.named_scope("prep"):
        prepare(0)
    for g in range(1, groups):
        wait_group(g)
    for g in range(groups):
        with jax.named_scope("place"):
            for j in range(GROUP):
                place(g, j)
                if g:
                    gather_sums(g - 1, range(j * per_cell, (j + 1) * per_cell))
                if j == 0 and g < groups - 1:
                    prepare(g + 1)
    with jax.named_scope("tail"):
        for j in range(GROUP):
            gather_sums(groups - 1, range(j * per_cell, (j + 1) * per_cell))
        for high in range(HIGHS):
            for stat, ref in enumerate((mean_rows, spare_rows)):
                line = ref[high * BLOCK:(high + 1) * BLOCK, :].astype(bf16)
                sums_ref[(high % hubs) * owners + high // hubs, stat * BLOCK:(stat + 1) * BLOCK, :] = line

    with jax.named_scope("barrier_wait"):
        pl.semaphore_wait(barrier, n - 1)
    with jax.named_scope("scatter_send"):
        each_hub(lambda slot, where: send(sums_ref.at[slot], got.at[me], 0, where))
    got[me] = sums_ref[hub * owners + z]

    with jax.named_scope("select"):
        share = dense_ref.shape[2]
        out_tiles = share // LANES
        chunk = min(256, share)
        pairs = HIGHS // 2
        for pair in range(pairs):
            at = 2 * pair * local
            line = jnp.concatenate([far_codes[at:at + local, :], far_codes[at + local:at + 2 * local, :]], axis=1)
            table[pair * local:(pair + 1) * local, :] = line.astype(bf16)
        chunk_ids = lax.broadcasted_iota(jnp.int32, (16, chunk), 0).astype(f32).astype(bf16)
        loads[1 + 2 * groups].wait()
        for first in range(0, owners * share, chunk):
            picked = selected_ref[:, first:first + chunk]
            inside = (lax.shift_right_logical(picked, 4) & (2 * LANES - 1)).astype(f32)
            inside = jnp.broadcast_to(inside, (16, chunk)).astype(bf16)
            one_hot = jnp.concatenate(
                [jnp.where(inside == chunk_ids + bf16(16 * k), bf16(1.0), bf16(0.0)) for k in range(16)], axis=0
            )
            found = jnp.dot(table[...], one_hot, preferred_element_type=f32)
            which = jnp.broadcast_to(lax.shift_right_logical(picked, 12), (local, chunk))
            mix = found[:local]
            for pair in range(1, pairs):
                mix = jnp.where(which == pair, found[local * pair:local * (pair + 1)], mix)
            value = mix * jnp.exp2((BASE - (picked & (BLOCK - 1)) * WIDTH).astype(f32))
            x = jnp.where((value > 2.0 ** -4.5) & (value < 2.0 ** 3.5), value, 0.0)
            owner, start = first // share, first % share
            dense_ref[owner, :, start:start + chunk] = x.astype(bf16)
            total = jnp.sum(x, axis=0, keepdims=True)
            square = jnp.sum(x * x, axis=0, keepdims=True)
            pair = jnp.concatenate([total, square], axis=0)
            for tile in range(chunk // LANES):
                at = (start // LANES + tile) * owners + owner
                sel_sums_ref[at] = pair[:, tile * LANES:(tile + 1) * LANES]

    with jax.named_scope("sel_send"):
        each_hub(lambda slot, where: send(sel_sums_ref.at[slot], sel_got.at[me], 1, where))

        def move(k, carry):
            owner = lax.rem(z + k, owners)
            send(dense_ref.at[owner], moved_ref.at[z], 2, {"gx": gx, "gy": gy, "gz": owner})
            return carry

        lax.fori_loop(1, owners, move, 0)
        sel_got[me] = sel_sums_ref[hub * owners + z]
        moved_ref[z] = dense_ref[z]

    @pl.when(is_hub)
    def _():
        with jax.named_scope("wait_rs"):
            finish(recv_sem.at[0], got, n - 1)
        with jax.named_scope("reduce"):
            means = got[:, :BLOCK, :].astype(f32)
            mean = jnp.sum(means, axis=0) * (1.0 / n)
            away = means - mean[None]
            spare = got[:, BLOCK:, :].astype(f32)
            variance = jnp.sum(spare + (away * away) * float(local), axis=0) * (1.0 / cells)
            turned[:LANES, :] = jnp.transpose(mean)
            turned[LANES:, :] = jnp.transpose(variance)
            pieces = [turned[pl.ds(k, lines, stride=LANES // BLOCK), :] for k in range(LANES // BLOCK)]
            mine[...] = jnp.concatenate(pieces, axis=1).astype(bf16)
        with jax.named_scope("gather_send"):
            each_team(lambda where: send(mine, stats_ref.at[hub], 3, where))
        with jax.named_scope("wait_selrs"):
            finish(recv_sem.at[1], sel_got, n - 1)
        with jax.named_scope("selreduce"):
            sel_mine[...] = jnp.sum(sel_got[...], axis=0)
            each_team(lambda where: send(sel_mine, sel_stats_ref.at[hub], 4, where))
            stats_ref[hub] = mine[...]
            sel_stats_ref[hub] = sel_mine[...]

    with jax.named_scope("wait_moved"):
        finish(recv_sem.at[2], moved_ref, owners - 1)
        finish(send_sem.at[2], moved_ref, owners - 1)

    @pl.when(is_hub)
    def _():
        finish(send_sem.at[0], sums_ref, hubs * owners - 1)
        finish(send_sem.at[1], sel_sums_ref, hubs * owners - 1)
        with jax.named_scope("wait_stats"):
            finish(recv_sem.at[3], stats_ref, hubs - 1)
        with jax.named_scope("wait_sel"):
            finish(recv_sem.at[4], sel_stats_ref, hubs - 1)
            for _ in range(teams - 1):
                finish(send_sem.at[3], stats_ref, 1)
                finish(send_sem.at[4], sel_stats_ref, 1)

    @pl.when(is_leaf)
    def _():
        finish(send_sem.at[0], sums_ref, hubs * owners)
        finish(send_sem.at[1], sel_sums_ref, hubs * owners)
        with jax.named_scope("wait_stats"):
            finish(recv_sem.at[3], stats_ref, hubs)
        with jax.named_scope("wait_sel"):
            finish(recv_sem.at[4], sel_stats_ref, hubs)


def final_kernel(cells, stats_ref, sel_stats_ref, moved_ref, gene_hbm, pca_hbm, gene_ref, pca_ref, sem):
    f32, bf16 = jnp.float32, jnp.bfloat16
    hubs, double, lanes = stats_ref.shape
    lines = double // 2
    stats = stats_ref[...].astype(f32)
    for hub in range(hubs):
        for stat in range(2):
            gene_ref[hub * lines:(hub + 1) * lines, stat, :] = stats[hub, stat * lines:(stat + 1) * lines]
    gene_copy = pltpu.make_async_copy(gene_ref, gene_hbm, sem.at[0])
    gene_copy.start()
    owners, local, share = moved_ref.shape
    tiles = share // lanes
    for tile in range(tiles):
        mean = sel_stats_ref[tile, 0:1, :] * (1.0 / cells)
        variance = sel_stats_ref[tile, 1:2, :] * (1.0 / cells) - mean * mean
        scale = 1.0 / jnp.sqrt(jnp.maximum(variance, var_floor))
        cols = slice(tile * lanes, (tile + 1) * lanes)
        for owner in range(owners):
            x = moved_ref[owner, :, cols].astype(f32)
            y = jnp.clip((x - mean) * scale, -clip_value, clip_value)
            pca_ref[owner * local:(owner + 1) * local, cols] = y.astype(bf16)
    pca_copy = pltpu.make_async_copy(pca_ref, pca_hbm, sem.at[1])
    pca_copy.start()
    gene_copy.wait()
    pca_copy.wait()


def per_device(sizes, columns, counts, nnz_count, selected):
    f32, bf16, i32 = jnp.float32, jnp.bfloat16, jnp.int32
    nx, ny, owners = sizes
    teams = nx * ny
    n = teams * owners
    local, slots = columns.shape
    hubs = HIGHS // owners
    across, along, step_x, step_y = hub_grid(nx, ny, hubs)
    share = selected.shape[0] // owners
    assert hubs * owners == HIGHS and across * along == hubs and across * step_x == nx and along * step_y == ny
    assert share == hubs * LANES and local % GROUP == 0
    hbm = pl.BlockSpec(memory_space=pltpu.HBM)
    vmem = pl.BlockSpec(memory_space=pltpu.VMEM)
    slot_rows = local * slots // LANES + 16
    far_rows = HIGHS * local
    arrays = (columns, counts, nnz_count.reshape(1, local), selected.reshape(1, -1))
    kept = pl.pallas_call(
        functools.partial(fused_kernel, sizes, local * n),
        name="moments_and_selection",
        out_shape=(
            pltpu.VMEM((hubs, 2 * BLOCK, LANES), bf16),
            pltpu.VMEM((hubs, 2, LANES), f32),
            pltpu.VMEM((owners, local, share), bf16),
        ),
        in_specs=[hbm] * 4,
        out_specs=(vmem,) * 3,
        scratch_shapes=[
            pltpu.VMEM((local, slots), i32),
            pltpu.VMEM((local, slots), i32),
            pltpu.VMEM((1, local), i32),
            pltpu.VMEM((1, owners * share), i32),
        ]
        + [pltpu.VMEM((slot_rows, LANES), f32)] * 3
        + [pltpu.VMEM((local, HIGHS, LANES), f32)] * 2
        + [pltpu.VMEM((far_rows, LANES), f32)]
        + [pltpu.VMEM((BLOCK, HIGHS, LANES), f32)] * 2
        + [pltpu.VMEM((far_rows // 2, 2 * LANES), bf16)]
        + [pltpu.VMEM((HIGHS * BLOCK, LANES), f32)] * 2
        + [
            pltpu.VMEM((HIGHS, 2 * BLOCK, LANES), bf16),
            pltpu.VMEM((HIGHS, 2, LANES), f32),
            pltpu.VMEM((owners, local, share), bf16),
            pltpu.VMEM((n, 2 * BLOCK, LANES), bf16),
            pltpu.VMEM((n, 2, LANES), f32),
            pltpu.VMEM((2 * BLOCK, LANES), bf16),
            pltpu.VMEM((2, LANES), f32),
            pltpu.VMEM((2 * LANES, BLOCK), f32),
            pltpu.SemaphoreType.DMA((2 + 2 * (local // GROUP),)),
            pltpu.SemaphoreType.DMA((5,)),
            pltpu.SemaphoreType.DMA((5,)),
        ],
        compiler_params=pltpu.CompilerParams(
            collective_id=0, has_side_effects=True, vmem_limit_bytes=32 * 1024 * 1024
        ),
    )(*(pltpu.with_memory_space_constraint(array, pltpu.HBM) for array in arrays))
    out_lines = GENES // owners // LANES
    gene_stats, pca_input = pl.pallas_call(
        functools.partial(final_kernel, local * n),
        name="standardize",
        out_shape=(pltpu.HBM((out_lines, 2, LANES), f32), pltpu.HBM((owners * local, share), bf16)),
        in_specs=[vmem] * 3,
        out_specs=(hbm,) * 2,
        scratch_shapes=[
            pltpu.VMEM((out_lines, 2, LANES), f32),
            pltpu.VMEM((owners * local, share), bf16),
            pltpu.SemaphoreType.DMA((2,)),
        ],
        compiler_params=pltpu.CompilerParams(vmem_limit_bytes=16 * 1024 * 1024),
    )(*(pltpu.with_memory_space_constraint(array, pltpu.VMEM) for array in kept))
    return (gene_stats.transpose(1, 0, 2).reshape(2, -1), pca_input)


def solution(mesh):
    sizes = tuple(mesh.shape[axis] for axis in ("gx", "gy", "gz"))
    return jax.shard_map(
        functools.partial(per_device, sizes),
        mesh=mesh,
        in_specs=(
            P(("gx", "gy", "gz"), None),
            P(("gx", "gy", "gz"), None),
            P(("gx", "gy", "gz")),
            P(),
        ),
        out_specs=(P(None, "gz"), P(("gx", "gy"), "gz")),
        check_vma=False,
    )
```

```python
import functools

import jax
import jax.numpy as jnp
from jax import lax
from jax.experimental import pallas as pl
from jax.experimental.pallas import tpu as pltpu
from jax.sharding import PartitionSpec as P

GENES = 32768
BLOCK = 16
LANES = 128
GROUP = 8
HIGHS = GENES // (BLOCK * LANES)
WIDTH = 8
BASE = 60
PARTS = 3
PART = -(-LANES // PARTS)

target_sum = 10000.0
var_floor = 0.01
clip_value = 10.0

MESH = pl.DeviceIdType.MESH


def flip(value, k, size):
    out, bit = 0, 1
    while bit < size:
        part = lax.rem(lax.div(value, bit), 2)
        out = out + (1 - part if k & bit else part) * bit
        bit *= 2
    return out


def hub_grid(nx, ny, count):
    across = max(1, count // ny)
    along = count // across
    return across, along, nx // across, ny // along


def fused_kernel(
    sizes, cells, columns_hbm, counts_hbm, nnz_hbm, selected_hbm, stats_ref, sel_stats_ref, moved_ref,
    columns_ref, counts_ref, nnz_ref, selected_ref, code_rows, high_rows, low_rows,
    near_values, near_offsets, far_codes, acc_values, acc_squares, table,
    mean_rows, spare_rows, sums_ref, sel_sums_ref, dense_ref, got, sel_got, mine, sel_mine, turned,
    load_sem, send_sem, recv_sem,
):
    nx, ny, owners = sizes
    teams = nx * ny
    n = teams * owners
    gx, gy, z = lax.axis_index("gx"), lax.axis_index("gy"), lax.axis_index("gz")
    r = gx * ny + gy
    me = r * owners + z
    bf16, f32 = jnp.bfloat16, jnp.float32
    local, slots = columns_ref.shape
    groups = local // GROUP
    tiles = slots // LANES
    hubs = HIGHS // owners
    across, along, step_x, step_y = hub_grid(nx, ny, hubs)
    hub_x, hub_y = lax.div(gx, step_x), lax.div(gy, step_y)
    hub = hub_x * along + hub_y
    is_hub = (gx == hub_x * step_x + step_x - 1) & (gy == hub_y * step_y + step_y - 1)
    is_leaf = jnp.logical_not(is_hub)
    lines = 2 * BLOCK

    loads = [pltpu.make_async_copy(nnz_hbm, nnz_ref, load_sem.at[0])]
    for g in range(groups):
        span = pl.ds(g * GROUP, GROUP)
        loads.append(pltpu.make_async_copy(counts_hbm.at[span], counts_ref.at[span], load_sem.at[1 + 2 * g]))
        loads.append(pltpu.make_async_copy(columns_hbm.at[span], columns_ref.at[span], load_sem.at[2 + 2 * g]))
    loads.append(pltpu.make_async_copy(selected_hbm, selected_ref, load_sem.at[1 + 2 * groups]))
    for load in loads:
        load.start()

    xs = [flip(gx, k, nx) for k in range(nx)]
    ys = [flip(gy, k, ny) for k in range(ny)]
    zs = [flip(z, k, owners) for k in range(owners)]
    hub_xs = [flip(hub_x, k, across) for k in range(across)]
    hub_ys = [flip(hub_y, k, along) for k in range(along)]

    def greet(where):
        pl.semaphore_signal(barrier, inc=1, device_id=where, device_id_type=MESH)

    def each_hub(act, kys):
        for ky in kys:
            for kx in reversed(range(across)):
                for kz in reversed(range(owners)):
                    hx, hy = hub_xs[kx], hub_ys[ky]
                    slot = (hx * along + hy) * owners + zs[kz]
                    where = {"gx": hx * step_x + step_x - 1, "gy": hy * step_y + step_y - 1, "gz": zs[kz]}
                    if ky or kx or kz:
                        act(slot, where)
                    else:
                        pl.when(is_leaf)(functools.partial(act, slot, where))

    steps = list(reversed(range(along)))
    far_steps, near_steps = steps[:along // 2], steps[along // 2:]

    def each_team(act):
        for ky in reversed(range(ny)):
            for kx in sorted(range(nx), key=lambda k: (k & 1, k), reverse=True):
                if ky or kx:
                    act({"gx": xs[kx], "gy": ys[ky], "gz": z})

    barrier = pltpu.get_barrier_semaphore()
    if n <= 64:
        for ky in reversed(range(ny)):
            for kx in reversed(range(nx)):
                for kz in reversed(range(owners)):
                    if ky or kx or kz:
                        greet({"gx": xs[kx], "gy": ys[ky], "gz": zs[kz]})
    else:
        def greet_step(k, carry):
            other = lax.rem(me + k, n)
            team, owner = lax.div(other, owners), lax.rem(other, owners)
            greet({"gx": lax.div(team, ny), "gy": lax.rem(team, ny), "gz": owner})
            return carry

        lax.fori_loop(1, n, greet_step, 0)

    def send(src, dst, kind, where):
        pltpu.make_async_remote_copy(
            src_ref=src, dst_ref=dst, send_sem=send_sem.at[kind], recv_sem=recv_sem.at[kind],
            device_id=where, device_id_type=MESH,
        ).start()

    def finish(sem, ref, count):
        if count:
            span = ref.at[pl.ds(0, count)]
            pltpu.make_async_copy(span, span, sem).wait()

    ids = lax.broadcasted_iota(jnp.int32, (16, slots), 0).astype(f32).astype(bf16)
    sub = lax.broadcasted_iota(jnp.int32, (GROUP, local), 0)
    lane = lax.broadcasted_iota(jnp.int32, (GROUP, local), 1)
    slot = lax.broadcasted_iota(jnp.int32, (GROUP, slots), 1)

    def wait_group(g):
        loads[1 + 2 * g].wait()
        loads[2 + 2 * g].wait()

    def prepare(g):
        span = slice(g * GROUP, (g + 1) * GROUP)
        live_count = jnp.sum(jnp.where(sub + g * GROUP == lane, nnz_ref[...], 0), axis=1, keepdims=True)
        live = slot < live_count
        raw = jnp.where(live, counts_ref[span, :].astype(f32), 0.0)
        library = jnp.sum(raw, axis=1, keepdims=True)
        value = jnp.log(1.0 + raw * (target_sum / library))
        genes = columns_ref[span, :]
        shift = ((genes & (BLOCK - 1)) * WIDTH - BASE).astype(f32)
        code = value * jnp.exp2(shift)
        high = lax.shift_right_logical(genes, 11)
        low = lax.shift_right_logical(genes, 4) & (LANES - 1)
        for k in range(1, PARTS):
            past = low >= PART
            high = high + jnp.where(past, HIGHS, 0)
            low = low - jnp.where(past, PART, 0)
        high, low = high.astype(f32), low.astype(f32)
        for tile in range(tiles):
            at = (g * tiles + tile) * GROUP
            cols = slice(tile * LANES, (tile + 1) * LANES)
            for ref, line in ((code_rows, code), (high_rows, high), (low_rows, low)):
                ref[at:at + GROUP, :] = line[:, cols]

    def spread(ref, g, j):
        return jnp.concatenate(
            [ref[pl.ds((g * tiles + tile) * GROUP + j, 16, stride=0), :].astype(bf16) for tile in range(tiles)],
            axis=1,
        )

    def place(g, j):
        c = g * GROUP + j
        zero, one = bf16(0.0), bf16(1.0)
        high, code, low = spread(high_rows, g, j), spread(code_rows, g, j), spread(low_rows, g, j)
        left = jnp.concatenate(
            [jnp.where(high == ids + bf16(HIGHS * k), code, zero) for k in range(PARTS)], axis=0
        )
        right = jnp.concatenate(
            [jnp.where(low == ids + bf16(16 * k), one, zero) for k in range(-(-PART // 16))], axis=0
        )
        placed = lax.dot_general(left, right, (((1,), (1,)), ((), ())), preferred_element_type=f32)
        pieces = [
            placed[HIGHS * k:HIGHS * (k + 1), :min(PART, LANES - k * PART)] for k in range(PARTS)
        ]
        code = jnp.concatenate(pieces, axis=1)
        far_codes[pl.ds(c, HIGHS, stride=local), :] = code
        power = jnp.log2(jnp.maximum(code, 2.0 ** (-BASE - WIDTH)))
        offset = jnp.floor((power + (BASE + 0.5 * WIDTH)) * (1.0 / WIDTH))
        value = code * jnp.exp2(BASE - WIDTH * offset)
        near_values[c], near_offsets[c] = value, offset

    def gather_sums(g, ks):
        total = [jnp.zeros((HIGHS, LANES), f32) if g == 0 else acc_values[k] for k in ks]
        square = [jnp.zeros((HIGHS, LANES), f32) if g == 0 else acc_squares[k] for k in ks]
        for j in range(GROUP):
            c = g * GROUP + j
            v, o = near_values[c], near_offsets[c]
            for i, k in enumerate(ks):
                hit = jnp.where(o == float(k), v, 0.0)
                total[i] = total[i] + hit
                square[i] = square[i] + hit * hit
        for i, k in enumerate(ks):
            if g < groups - 1:
                acc_values[k], acc_squares[k] = total[i], square[i]
                continue
            near = total[i] * (1.0 / local)
            mean_rows[pl.ds(k, HIGHS, stride=BLOCK), :] = near
            spare_rows[pl.ds(k, HIGHS, stride=BLOCK), :] = square[i] - total[i] * near

    per_cell = BLOCK // GROUP
    loads[0].wait()
    wait_group(0)
    with jax.named_scope("prep"):
        prepare(0)
    for g in range(1, groups):
        wait_group(g)
    for g in range(groups):
        with jax.named_scope("place"):
            for j in range(GROUP):
                place(g, j)
                if g:
                    gather_sums(g - 1, range(j * per_cell, (j + 1) * per_cell))
                if j == 0 and g < groups - 1:
                    prepare(g + 1)
    with jax.named_scope("tail"):
        for j in range(GROUP):
            gather_sums(groups - 1, range(j * per_cell, (j + 1) * per_cell))
        for high in range(HIGHS):
            for stat, ref in enumerate((mean_rows, spare_rows)):
                line = ref[high * BLOCK:(high + 1) * BLOCK, :].astype(bf16)
                sums_ref[(high % hubs) * owners + high // hubs, stat * BLOCK:(stat + 1) * BLOCK, :] = line

    with jax.named_scope("barrier_wait"):
        pl.semaphore_wait(barrier, n - 1)
    with jax.named_scope("scatter_send"):
        each_hub(lambda slot, where: send(sums_ref.at[slot], got.at[me], 0, where), far_steps)
    got[me] = sums_ref[hub * owners + z]

    with jax.named_scope("select"):
        share = dense_ref.shape[2]
        out_tiles = share // LANES
        chunk = min(256, share)
        pairs = HIGHS // 2
        for pair in range(pairs):
            at = 2 * pair * local
            line = jnp.concatenate([far_codes[at:at + local, :], far_codes[at + local:at + 2 * local, :]], axis=1)
            table[pair * local:(pair + 1) * local, :] = line.astype(bf16)
        chunk_ids = lax.broadcasted_iota(jnp.int32, (16, chunk), 0).astype(f32).astype(bf16)
        loads[1 + 2 * groups].wait()
        for first in range(0, owners * share, chunk):
            picked = selected_ref[:, first:first + chunk]
            inside = (lax.shift_right_logical(picked, 4) & (2 * LANES - 1)).astype(f32)
            inside = jnp.broadcast_to(inside, (16, chunk)).astype(bf16)
            one_hot = jnp.concatenate(
                [jnp.where(inside == chunk_ids + bf16(16 * k), bf16(1.0), bf16(0.0)) for k in range(16)], axis=0
            )
            found = jnp.dot(table[...], one_hot, preferred_element_type=f32)
            which = jnp.broadcast_to(lax.shift_right_logical(picked, 12), (local, chunk))
            mix = found[:local]
            for pair in range(1, pairs):
                mix = jnp.where(which == pair, found[local * pair:local * (pair + 1)], mix)
            value = mix * jnp.exp2((BASE - (picked & (BLOCK - 1)) * WIDTH).astype(f32))
            x = jnp.where((value > 2.0 ** -4.5) & (value < 2.0 ** 3.5), value, 0.0)
            owner, start = first // share, first % share
            dense_ref[owner, :, start:start + chunk] = x.astype(bf16)
            total = jnp.sum(x, axis=0, keepdims=True)
            square = jnp.sum(x * x, axis=0, keepdims=True)
            pair = jnp.concatenate([total, square], axis=0)
            for tile in range(chunk // LANES):
                at = (start // LANES + tile) * owners + owner
                sel_sums_ref[at] = pair[:, tile * LANES:(tile + 1) * LANES]

    with jax.named_scope("sel_send"):
        each_hub(lambda slot, where: send(sel_sums_ref.at[slot], sel_got.at[me], 1, where), far_steps + near_steps)
        each_hub(lambda slot, where: send(sums_ref.at[slot], got.at[me], 0, where), near_steps)

        def move(k, carry):
            owner = lax.rem(z + k, owners)
            send(dense_ref.at[owner], moved_ref.at[z], 2, {"gx": gx, "gy": gy, "gz": owner})
            return carry

        lax.fori_loop(1, owners, move, 0)
        sel_got[me] = sel_sums_ref[hub * owners + z]
        moved_ref[z] = dense_ref[z]

    @pl.when(is_hub)
    def _():
        with jax.named_scope("wait_selrs"):
            finish(recv_sem.at[1], sel_got, n - 1)
        with jax.named_scope("selreduce"):
            sel_mine[...] = jnp.sum(sel_got[...], axis=0)
            each_team(lambda where: send(sel_mine, sel_stats_ref.at[hub], 4, where))
            sel_stats_ref[hub] = sel_mine[...]
        with jax.named_scope("wait_rs"):
            finish(recv_sem.at[0], got, n - 1)
        with jax.named_scope("reduce"):
            means = got[:, :BLOCK, :].astype(f32)
            mean = jnp.sum(means, axis=0) * (1.0 / n)
            away = means - mean[None]
            spare = got[:, BLOCK:, :].astype(f32)
            variance = jnp.sum(spare + (away * away) * float(local), axis=0) * (1.0 / cells)
            turned[:LANES, :] = jnp.transpose(mean)
            turned[LANES:, :] = jnp.transpose(variance)
            pieces = [turned[pl.ds(k, lines, stride=LANES // BLOCK), :] for k in range(LANES // BLOCK)]
            mine[...] = jnp.concatenate(pieces, axis=1).astype(bf16)
        with jax.named_scope("gather_send"):
            each_team(lambda where: send(mine, stats_ref.at[hub], 3, where))
            stats_ref[hub] = mine[...]

    with jax.named_scope("wait_moved"):
        finish(recv_sem.at[2], moved_ref, owners - 1)
        finish(send_sem.at[2], moved_ref, owners - 1)

    @pl.when(is_hub)
    def _():
        finish(send_sem.at[0], sums_ref, hubs * owners - 1)
        finish(send_sem.at[1], sel_sums_ref, hubs * owners - 1)
        with jax.named_scope("wait_stats"):
            finish(recv_sem.at[3], stats_ref, hubs - 1)
        with jax.named_scope("wait_sel"):
            finish(recv_sem.at[4], sel_stats_ref, hubs - 1)
            for _ in range(teams - 1):
                finish(send_sem.at[3], stats_ref, 1)
                finish(send_sem.at[4], sel_stats_ref, 1)

    @pl.when(is_leaf)
    def _():
        finish(send_sem.at[0], sums_ref, hubs * owners)
        finish(send_sem.at[1], sel_sums_ref, hubs * owners)
        with jax.named_scope("wait_stats"):
            finish(recv_sem.at[3], stats_ref, hubs)
        with jax.named_scope("wait_sel"):
            finish(recv_sem.at[4], sel_stats_ref, hubs)


def final_kernel(cells, stats_ref, sel_stats_ref, moved_ref, gene_hbm, pca_hbm, gene_ref, pca_ref, sem):
    f32, bf16 = jnp.float32, jnp.bfloat16
    hubs, double, lanes = stats_ref.shape
    lines = double // 2
    stats = stats_ref[...].astype(f32)
    for hub in range(hubs):
        for stat in range(2):
            gene_ref[hub * lines:(hub + 1) * lines, stat, :] = stats[hub, stat * lines:(stat + 1) * lines]
    gene_copy = pltpu.make_async_copy(gene_ref, gene_hbm, sem.at[0])
    gene_copy.start()
    owners, local, share = moved_ref.shape
    tiles = share // lanes
    for tile in range(tiles):
        mean = sel_stats_ref[tile, 0:1, :] * (1.0 / cells)
        variance = sel_stats_ref[tile, 1:2, :] * (1.0 / cells) - mean * mean
        scale = 1.0 / jnp.sqrt(jnp.maximum(variance, var_floor))
        cols = slice(tile * lanes, (tile + 1) * lanes)
        for owner in range(owners):
            x = moved_ref[owner, :, cols].astype(f32)
            y = jnp.clip((x - mean) * scale, -clip_value, clip_value)
            pca_ref[owner * local:(owner + 1) * local, cols] = y.astype(bf16)
    pca_copy = pltpu.make_async_copy(pca_ref, pca_hbm, sem.at[1])
    pca_copy.start()
    gene_copy.wait()
    pca_copy.wait()


def per_device(sizes, columns, counts, nnz_count, selected):
    f32, bf16, i32 = jnp.float32, jnp.bfloat16, jnp.int32
    nx, ny, owners = sizes
    teams = nx * ny
    n = teams * owners
    local, slots = columns.shape
    hubs = HIGHS // owners
    across, along, step_x, step_y = hub_grid(nx, ny, hubs)
    share = selected.shape[0] // owners
    assert hubs * owners == HIGHS and across * along == hubs and across * step_x == nx and along * step_y == ny
    assert share == hubs * LANES and local % GROUP == 0
    hbm = pl.BlockSpec(memory_space=pltpu.HBM)
    vmem = pl.BlockSpec(memory_space=pltpu.VMEM)
    slot_rows = local * slots // LANES + 16
    far_rows = HIGHS * local
    arrays = (columns, counts, nnz_count.reshape(1, local), selected.reshape(1, -1))
    kept = pl.pallas_call(
        functools.partial(fused_kernel, sizes, local * n),
        name="moments_and_selection",
        out_shape=(
            pltpu.VMEM((hubs, 2 * BLOCK, LANES), bf16),
            pltpu.VMEM((hubs, 2, LANES), f32),
            pltpu.VMEM((owners, local, share), bf16),
        ),
        in_specs=[hbm] * 4,
        out_specs=(vmem,) * 3,
        scratch_shapes=[
            pltpu.VMEM((local, slots), i32),
            pltpu.VMEM((local, slots), i32),
            pltpu.VMEM((1, local), i32),
            pltpu.VMEM((1, owners * share), i32),
        ]
        + [pltpu.VMEM((slot_rows, LANES), f32)] * 3
        + [pltpu.VMEM((local, HIGHS, LANES), f32)] * 2
        + [pltpu.VMEM((far_rows, LANES), f32)]
        + [pltpu.VMEM((BLOCK, HIGHS, LANES), f32)] * 2
        + [pltpu.VMEM((far_rows // 2, 2 * LANES), bf16)]
        + [pltpu.VMEM((HIGHS * BLOCK, LANES), f32)] * 2
        + [
            pltpu.VMEM((HIGHS, 2 * BLOCK, LANES), bf16),
            pltpu.VMEM((HIGHS, 2, LANES), f32),
            pltpu.VMEM((owners, local, share), bf16),
            pltpu.VMEM((n, 2 * BLOCK, LANES), bf16),
            pltpu.VMEM((n, 2, LANES), f32),
            pltpu.VMEM((2 * BLOCK, LANES), bf16),
            pltpu.VMEM((2, LANES), f32),
            pltpu.VMEM((2 * LANES, BLOCK), f32),
            pltpu.SemaphoreType.DMA((2 + 2 * (local // GROUP),)),
            pltpu.SemaphoreType.DMA((5,)),
            pltpu.SemaphoreType.DMA((5,)),
        ],
        compiler_params=pltpu.CompilerParams(
            collective_id=0, has_side_effects=True, vmem_limit_bytes=32 * 1024 * 1024
        ),
    )(*(pltpu.with_memory_space_constraint(array, pltpu.HBM) for array in arrays))
    out_lines = GENES // owners // LANES
    gene_stats, pca_input = pl.pallas_call(
        functools.partial(final_kernel, local * n),
        name="standardize",
        out_shape=(pltpu.HBM((out_lines, 2, LANES), f32), pltpu.HBM((owners * local, share), bf16)),
        in_specs=[vmem] * 3,
        out_specs=(hbm,) * 2,
        scratch_shapes=[
            pltpu.VMEM((out_lines, 2, LANES), f32),
            pltpu.VMEM((owners * local, share), bf16),
            pltpu.SemaphoreType.DMA((2,)),
        ],
        compiler_params=pltpu.CompilerParams(vmem_limit_bytes=16 * 1024 * 1024),
    )(*(pltpu.with_memory_space_constraint(array, pltpu.VMEM) for array in kept))
    return (gene_stats.transpose(1, 0, 2).reshape(2, -1), pca_input)


def solution(mesh):
    sizes = tuple(mesh.shape[axis] for axis in ("gx", "gy", "gz"))
    return jax.shard_map(
        functools.partial(per_device, sizes),
        mesh=mesh,
        in_specs=(
            P(("gx", "gy", "gz"), None),
            P(("gx", "gy", "gz"), None),
            P(("gx", "gy", "gz")),
            P(),
        ),
        out_specs=(P(None, "gz"), P(("gx", "gy"), "gz")),
        check_vma=False,
    )
```

```python
import functools

import jax
import jax.numpy as jnp
from jax import lax
from jax.experimental import pallas as pl
from jax.experimental.pallas import tpu as pltpu
from jax.sharding import PartitionSpec as P

GENES = 32768
BLOCK = 16
LANES = 128
GROUP = 8
HIGHS = GENES // (BLOCK * LANES)
WIDTH = 8
BASE = 60
PARTS = 3
PART = -(-LANES // PARTS)

target_sum = 10000.0
var_floor = 0.01
clip_value = 10.0

MESH = pl.DeviceIdType.MESH


def flip(value, k, size):
    out, bit = 0, 1
    while bit < size:
        part = lax.rem(lax.div(value, bit), 2)
        out = out + (1 - part if k & bit else part) * bit
        bit *= 2
    return out


def hub_grid(nx, ny, count):
    across = max(1, count // ny)
    along = count // across
    return across, along, nx // across, ny // along


def fused_kernel(
    sizes, cells, columns_hbm, counts_hbm, nnz_hbm, selected_hbm, stats_ref, sel_stats_ref, moved_ref,
    columns_ref, counts_ref, nnz_ref, selected_ref, code_rows, high_rows, low_rows,
    near_values, near_offsets, far_codes, acc_values, acc_squares, table,
    mean_rows, spare_rows, sums_ref, sel_sums_ref, dense_ref, got, sel_got, mine, sel_mine, turned,
    load_sem, send_sem, recv_sem,
):
    nx, ny, owners = sizes
    teams = nx * ny
    n = teams * owners
    gx, gy, z = lax.axis_index("gx"), lax.axis_index("gy"), lax.axis_index("gz")
    r = gx * ny + gy
    me = r * owners + z
    bf16, f32 = jnp.bfloat16, jnp.float32
    local, slots = columns_ref.shape
    groups = local // GROUP
    tiles = slots // LANES
    hubs = HIGHS // owners
    across, along, step_x, step_y = hub_grid(nx, ny, hubs)
    hub_x, hub_y = lax.div(gx, step_x), lax.div(gy, step_y)
    hub = hub_x * along + hub_y
    is_hub = (gx == hub_x * step_x + step_x - 1) & (gy == hub_y * step_y + step_y - 1)
    is_leaf = jnp.logical_not(is_hub)
    lines = 2 * BLOCK

    loads = [pltpu.make_async_copy(nnz_hbm, nnz_ref, load_sem.at[0])]
    for g in range(groups):
        span = pl.ds(g * GROUP, GROUP)
        loads.append(pltpu.make_async_copy(counts_hbm.at[span], counts_ref.at[span], load_sem.at[1 + 2 * g]))
        loads.append(pltpu.make_async_copy(columns_hbm.at[span], columns_ref.at[span], load_sem.at[2 + 2 * g]))
    loads.append(pltpu.make_async_copy(selected_hbm, selected_ref, load_sem.at[1 + 2 * groups]))
    for load in loads:
        load.start()

    xs = [flip(gx, k, nx) for k in range(nx)]
    ys = [flip(gy, k, ny) for k in range(ny)]
    zs = [flip(z, k, owners) for k in range(owners)]
    hub_xs = [flip(hub_x, k, across) for k in range(across)]
    hub_ys = [flip(hub_y, k, along) for k in range(along)]

    def greet(where):
        pl.semaphore_signal(barrier, inc=1, device_id=where, device_id_type=MESH)

    def each_hub(act, kys):
        for ky in kys:
            for kx in reversed(range(across)):
                for kz in reversed(range(owners)):
                    hx, hy = hub_xs[kx], hub_ys[ky]
                    slot = (hx * along + hy) * owners + zs[kz]
                    where = {"gx": hx * step_x + step_x - 1, "gy": hy * step_y + step_y - 1, "gz": zs[kz]}
                    if ky or kx or kz:
                        act(slot, where)
                    else:
                        pl.when(is_leaf)(functools.partial(act, slot, where))

    steps = list(reversed(range(along)))
    far_steps, near_steps = steps[:along // 2], steps[along // 2:]

    def each_team(act):
        for y in range(ny):
            for kx in sorted(range(nx), key=lambda k: (k & 1, k), reverse=True):
                if kx:
                    act({"gx": xs[kx], "gy": y, "gz": z})
                else:
                    pl.when(gy != y)(functools.partial(act, {"gx": gx, "gy": y, "gz": z}))

    barrier = pltpu.get_barrier_semaphore()
    if n <= 64:
        for ky in reversed(range(ny)):
            for kx in reversed(range(nx)):
                for kz in reversed(range(owners)):
                    if ky or kx or kz:
                        greet({"gx": xs[kx], "gy": ys[ky], "gz": zs[kz]})
    else:
        def greet_step(k, carry):
            other = lax.rem(me + k, n)
            team, owner = lax.div(other, owners), lax.rem(other, owners)
            greet({"gx": lax.div(team, ny), "gy": lax.rem(team, ny), "gz": owner})
            return carry

        lax.fori_loop(1, n, greet_step, 0)

    def send(src, dst, kind, where):
        pltpu.make_async_remote_copy(
            src_ref=src, dst_ref=dst, send_sem=send_sem.at[kind], recv_sem=recv_sem.at[kind],
            device_id=where, device_id_type=MESH,
        ).start()

    def finish(sem, ref, count):
        if count:
            span = ref.at[pl.ds(0, count)]
            pltpu.make_async_copy(span, span, sem).wait()

    ids = lax.broadcasted_iota(jnp.int32, (16, slots), 0).astype(f32).astype(bf16)
    sub = lax.broadcasted_iota(jnp.int32, (GROUP, local), 0)
    lane = lax.broadcasted_iota(jnp.int32, (GROUP, local), 1)
    slot = lax.broadcasted_iota(jnp.int32, (GROUP, slots), 1)

    def wait_group(g):
        loads[1 + 2 * g].wait()
        loads[2 + 2 * g].wait()

    def prepare(g):
        span = slice(g * GROUP, (g + 1) * GROUP)
        live_count = jnp.sum(jnp.where(sub + g * GROUP == lane, nnz_ref[...], 0), axis=1, keepdims=True)
        live = slot < live_count
        raw = jnp.where(live, counts_ref[span, :].astype(f32), 0.0)
        library = jnp.sum(raw, axis=1, keepdims=True)
        value = jnp.log(1.0 + raw * (target_sum / library))
        genes = columns_ref[span, :]
        shift = ((genes & (BLOCK - 1)) * WIDTH - BASE).astype(f32)
        code = value * jnp.exp2(shift)
        high = lax.shift_right_logical(genes, 11)
        low = lax.shift_right_logical(genes, 4) & (LANES - 1)
        for k in range(1, PARTS):
            past = low >= PART
            high = high + jnp.where(past, HIGHS, 0)
            low = low - jnp.where(past, PART, 0)
        high, low = high.astype(f32), low.astype(f32)
        for tile in range(tiles):
            at = (g * tiles + tile) * GROUP
            cols = slice(tile * LANES, (tile + 1) * LANES)
            for ref, line in ((code_rows, code), (high_rows, high), (low_rows, low)):
                ref[at:at + GROUP, :] = line[:, cols]

    def spread(ref, g, j):
        return jnp.concatenate(
            [ref[pl.ds((g * tiles + tile) * GROUP + j, 16, stride=0), :].astype(bf16) for tile in range(tiles)],
            axis=1,
        )

    def place(g, j):
        c = g * GROUP + j
        zero, one = bf16(0.0), bf16(1.0)
        high, code, low = spread(high_rows, g, j), spread(code_rows, g, j), spread(low_rows, g, j)
        left = jnp.concatenate(
            [jnp.where(high == ids + bf16(HIGHS * k), code, zero) for k in range(PARTS)], axis=0
        )
        right = jnp.concatenate(
            [jnp.where(low == ids + bf16(16 * k), one, zero) for k in range(-(-PART // 16))], axis=0
        )
        placed = lax.dot_general(left, right, (((1,), (1,)), ((), ())), preferred_element_type=f32)
        pieces = [
            placed[HIGHS * k:HIGHS * (k + 1), :min(PART, LANES - k * PART)] for k in range(PARTS)
        ]
        code = jnp.concatenate(pieces, axis=1)
        far_codes[pl.ds(c, HIGHS, stride=local), :] = code
        power = jnp.log2(jnp.maximum(code, 2.0 ** (-BASE - WIDTH)))
        offset = jnp.floor((power + (BASE + 0.5 * WIDTH)) * (1.0 / WIDTH))
        value = code * jnp.exp2(BASE - WIDTH * offset)
        near_values[c], near_offsets[c] = value, offset

    def gather_sums(g, ks):
        total = [jnp.zeros((HIGHS, LANES), f32) if g == 0 else acc_values[k] for k in ks]
        square = [jnp.zeros((HIGHS, LANES), f32) if g == 0 else acc_squares[k] for k in ks]
        for j in range(GROUP):
            c = g * GROUP + j
            v, o = near_values[c], near_offsets[c]
            for i, k in enumerate(ks):
                hit = jnp.where(o == float(k), v, 0.0)
                total[i] = total[i] + hit
                square[i] = square[i] + hit * hit
        for i, k in enumerate(ks):
            if g < groups - 1:
                acc_values[k], acc_squares[k] = total[i], square[i]
                continue
            near = total[i] * (1.0 / local)
            mean_rows[pl.ds(k, HIGHS, stride=BLOCK), :] = near
            spare_rows[pl.ds(k, HIGHS, stride=BLOCK), :] = square[i] - total[i] * near

    per_cell = BLOCK // GROUP
    loads[0].wait()
    wait_group(0)
    with jax.named_scope("prep"):
        prepare(0)
    for g in range(1, groups):
        wait_group(g)
    for g in range(groups):
        with jax.named_scope("place"):
            for j in range(GROUP):
                place(g, j)
                if g:
                    gather_sums(g - 1, range(j * per_cell, (j + 1) * per_cell))
                if j == 0 and g < groups - 1:
                    prepare(g + 1)
    with jax.named_scope("tail"):
        for j in range(GROUP):
            gather_sums(groups - 1, range(j * per_cell, (j + 1) * per_cell))
        for high in range(HIGHS):
            for stat, ref in enumerate((mean_rows, spare_rows)):
                line = ref[high * BLOCK:(high + 1) * BLOCK, :].astype(bf16)
                sums_ref[(high % hubs) * owners + high // hubs, stat * BLOCK:(stat + 1) * BLOCK, :] = line

    with jax.named_scope("barrier_wait"):
        pl.semaphore_wait(barrier, n - 1)
    with jax.named_scope("scatter_send"):
        each_hub(lambda slot, where: send(sums_ref.at[slot], got.at[me], 0, where), far_steps)
    got[me] = sums_ref[hub * owners + z]

    with jax.named_scope("select"):
        share = dense_ref.shape[2]
        out_tiles = share // LANES
        chunk = min(256, share)
        pairs = HIGHS // 2
        for pair in range(pairs):
            at = 2 * pair * local
            line = jnp.concatenate([far_codes[at:at + local, :], far_codes[at + local:at + 2 * local, :]], axis=1)
            table[pair * local:(pair + 1) * local, :] = line.astype(bf16)
        chunk_ids = lax.broadcasted_iota(jnp.int32, (16, chunk), 0).astype(f32).astype(bf16)
        loads[1 + 2 * groups].wait()
        for first in range(0, owners * share, chunk):
            picked = selected_ref[:, first:first + chunk]
            inside = (lax.shift_right_logical(picked, 4) & (2 * LANES - 1)).astype(f32)
            inside = jnp.broadcast_to(inside, (16, chunk)).astype(bf16)
            one_hot = jnp.concatenate(
                [jnp.where(inside == chunk_ids + bf16(16 * k), bf16(1.0), bf16(0.0)) for k in range(16)], axis=0
            )
            found = jnp.dot(table[...], one_hot, preferred_element_type=f32)
            which = jnp.broadcast_to(lax.shift_right_logical(picked, 12), (local, chunk))
            mix = found[:local]
            for pair in range(1, pairs):
                mix = jnp.where(which == pair, found[local * pair:local * (pair + 1)], mix)
            value = mix * jnp.exp2((BASE - (picked & (BLOCK - 1)) * WIDTH).astype(f32))
            x = jnp.where((value > 2.0 ** -4.5) & (value < 2.0 ** 3.5), value, 0.0)
            owner, start = first // share, first % share
            dense_ref[owner, :, start:start + chunk] = x.astype(bf16)
            total = jnp.sum(x, axis=0, keepdims=True)
            square = jnp.sum(x * x, axis=0, keepdims=True)
            pair = jnp.concatenate([total, square], axis=0)
            for tile in range(chunk // LANES):
                at = (start // LANES + tile) * owners + owner
                sel_sums_ref[at] = pair[:, tile * LANES:(tile + 1) * LANES]

    with jax.named_scope("sel_send"):
        each_hub(lambda slot, where: send(sel_sums_ref.at[slot], sel_got.at[me], 1, where), far_steps + near_steps)
        each_hub(lambda slot, where: send(sums_ref.at[slot], got.at[me], 0, where), near_steps)

        def move(k, carry):
            owner = lax.rem(z + k, owners)
            send(dense_ref.at[owner], moved_ref.at[z], 2, {"gx": gx, "gy": gy, "gz": owner})
            return carry

        lax.fori_loop(1, owners, move, 0)
        sel_got[me] = sel_sums_ref[hub * owners + z]
        moved_ref[z] = dense_ref[z]

    @pl.when(is_hub)
    def _():
        with jax.named_scope("wait_rs"):
            finish(recv_sem.at[0], got, n - 1)
        with jax.named_scope("reduce"):
            means = got[:, :BLOCK, :].astype(f32)
            mean = jnp.sum(means, axis=0) * (1.0 / n)
            away = means - mean[None]
            spare = got[:, BLOCK:, :].astype(f32)
            variance = jnp.sum(spare + (away * away) * float(local), axis=0) * (1.0 / cells)
            turned[:LANES, :] = jnp.transpose(mean)
            turned[LANES:, :] = jnp.transpose(variance)
            pieces = [turned[pl.ds(k, lines, stride=LANES // BLOCK), :] for k in range(LANES // BLOCK)]
            mine[...] = jnp.concatenate(pieces, axis=1).astype(bf16)
        with jax.named_scope("wait_selrs"):
            finish(recv_sem.at[1], sel_got, n - 1)
        with jax.named_scope("selreduce"):
            sel_mine[...] = jnp.sum(sel_got[...], axis=0)
            each_team(lambda where: send(sel_mine, sel_stats_ref.at[hub], 4, where))
            sel_stats_ref[hub] = sel_mine[...]
        with jax.named_scope("gather_send"):
            each_team(lambda where: send(mine, stats_ref.at[hub], 3, where))
            stats_ref[hub] = mine[...]

    with jax.named_scope("wait_moved"):
        finish(recv_sem.at[2], moved_ref, owners - 1)
        finish(send_sem.at[2], moved_ref, owners - 1)

    @pl.when(is_hub)
    def _():
        finish(send_sem.at[0], sums_ref, hubs * owners - 1)
        finish(send_sem.at[1], sel_sums_ref, hubs * owners - 1)
        with jax.named_scope("wait_stats"):
            finish(recv_sem.at[3], stats_ref, hubs - 1)
        with jax.named_scope("wait_sel"):
            finish(recv_sem.at[4], sel_stats_ref, hubs - 1)
            for _ in range(teams - 1):
                finish(send_sem.at[3], stats_ref, 1)
                finish(send_sem.at[4], sel_stats_ref, 1)

    @pl.when(is_leaf)
    def _():
        finish(send_sem.at[0], sums_ref, hubs * owners)
        finish(send_sem.at[1], sel_sums_ref, hubs * owners)
        with jax.named_scope("wait_stats"):
            finish(recv_sem.at[3], stats_ref, hubs)
        with jax.named_scope("wait_sel"):
            finish(recv_sem.at[4], sel_stats_ref, hubs)


def final_kernel(cells, stats_ref, sel_stats_ref, moved_ref, gene_hbm, pca_hbm, gene_ref, pca_ref, sem):
    f32, bf16 = jnp.float32, jnp.bfloat16
    hubs, double, lanes = stats_ref.shape
    lines = double // 2
    stats = stats_ref[...].astype(f32)
    for hub in range(hubs):
        for stat in range(2):
            gene_ref[hub * lines:(hub + 1) * lines, stat, :] = stats[hub, stat * lines:(stat + 1) * lines]
    gene_copy = pltpu.make_async_copy(gene_ref, gene_hbm, sem.at[0])
    gene_copy.start()
    owners, local, share = moved_ref.shape
    tiles = share // lanes
    for tile in range(tiles):
        mean = sel_stats_ref[tile, 0:1, :] * (1.0 / cells)
        variance = sel_stats_ref[tile, 1:2, :] * (1.0 / cells) - mean * mean
        scale = 1.0 / jnp.sqrt(jnp.maximum(variance, var_floor))
        cols = slice(tile * lanes, (tile + 1) * lanes)
        for owner in range(owners):
            x = moved_ref[owner, :, cols].astype(f32)
            y = jnp.clip((x - mean) * scale, -clip_value, clip_value)
            pca_ref[owner * local:(owner + 1) * local, cols] = y.astype(bf16)
    pca_copy = pltpu.make_async_copy(pca_ref, pca_hbm, sem.at[1])
    pca_copy.start()
    gene_copy.wait()
    pca_copy.wait()


def per_device(sizes, columns, counts, nnz_count, selected):
    f32, bf16, i32 = jnp.float32, jnp.bfloat16, jnp.int32
    nx, ny, owners = sizes
    teams = nx * ny
    n = teams * owners
    local, slots = columns.shape
    hubs = HIGHS // owners
    across, along, step_x, step_y = hub_grid(nx, ny, hubs)
    share = selected.shape[0] // owners
    assert hubs * owners == HIGHS and across * along == hubs and across * step_x == nx and along * step_y == ny
    assert share == hubs * LANES and local % GROUP == 0
    hbm = pl.BlockSpec(memory_space=pltpu.HBM)
    vmem = pl.BlockSpec(memory_space=pltpu.VMEM)
    slot_rows = local * slots // LANES + 16
    far_rows = HIGHS * local
    arrays = (columns, counts, nnz_count.reshape(1, local), selected.reshape(1, -1))
    kept = pl.pallas_call(
        functools.partial(fused_kernel, sizes, local * n),
        name="moments_and_selection",
        out_shape=(
            pltpu.VMEM((hubs, 2 * BLOCK, LANES), bf16),
            pltpu.VMEM((hubs, 2, LANES), f32),
            pltpu.VMEM((owners, local, share), bf16),
        ),
        in_specs=[hbm] * 4,
        out_specs=(vmem,) * 3,
        scratch_shapes=[
            pltpu.VMEM((local, slots), i32),
            pltpu.VMEM((local, slots), i32),
            pltpu.VMEM((1, local), i32),
            pltpu.VMEM((1, owners * share), i32),
        ]
        + [pltpu.VMEM((slot_rows, LANES), f32)] * 3
        + [pltpu.VMEM((local, HIGHS, LANES), f32)] * 2
        + [pltpu.VMEM((far_rows, LANES), f32)]
        + [pltpu.VMEM((BLOCK, HIGHS, LANES), f32)] * 2
        + [pltpu.VMEM((far_rows // 2, 2 * LANES), bf16)]
        + [pltpu.VMEM((HIGHS * BLOCK, LANES), f32)] * 2
        + [
            pltpu.VMEM((HIGHS, 2 * BLOCK, LANES), bf16),
            pltpu.VMEM((HIGHS, 2, LANES), f32),
            pltpu.VMEM((owners, local, share), bf16),
            pltpu.VMEM((n, 2 * BLOCK, LANES), bf16),
            pltpu.VMEM((n, 2, LANES), f32),
            pltpu.VMEM((2 * BLOCK, LANES), bf16),
            pltpu.VMEM((2, LANES), f32),
            pltpu.VMEM((2 * LANES, BLOCK), f32),
            pltpu.SemaphoreType.DMA((2 + 2 * (local // GROUP),)),
            pltpu.SemaphoreType.DMA((5,)),
            pltpu.SemaphoreType.DMA((5,)),
        ],
        compiler_params=pltpu.CompilerParams(
            collective_id=0, has_side_effects=True, vmem_limit_bytes=32 * 1024 * 1024
        ),
    )(*(pltpu.with_memory_space_constraint(array, pltpu.HBM) for array in arrays))
    out_lines = GENES // owners // LANES
    gene_stats, pca_input = pl.pallas_call(
        functools.partial(final_kernel, local * n),
        name="standardize",
        out_shape=(pltpu.HBM((out_lines, 2, LANES), f32), pltpu.HBM((owners * local, share), bf16)),
        in_specs=[vmem] * 3,
        out_specs=(hbm,) * 2,
        scratch_shapes=[
            pltpu.VMEM((out_lines, 2, LANES), f32),
            pltpu.VMEM((owners * local, share), bf16),
            pltpu.SemaphoreType.DMA((2,)),
        ],
        compiler_params=pltpu.CompilerParams(vmem_limit_bytes=16 * 1024 * 1024),
    )(*(pltpu.with_memory_space_constraint(array, pltpu.VMEM) for array in kept))
    return (gene_stats.transpose(1, 0, 2).reshape(2, -1), pca_input)


def solution(mesh):
    sizes = tuple(mesh.shape[axis] for axis in ("gx", "gy", "gz"))
    return jax.shard_map(
        functools.partial(per_device, sizes),
        mesh=mesh,
        in_specs=(
            P(("gx", "gy", "gz"), None),
            P(("gx", "gy", "gz"), None),
            P(("gx", "gy", "gz")),
            P(),
        ),
        out_specs=(P(None, "gz"), P(("gx", "gy"), "gz")),
        check_vma=False,
    )
```

```python
import functools

import jax
import jax.numpy as jnp
from jax import lax
from jax.experimental import pallas as pl
from jax.experimental.pallas import tpu as pltpu
from jax.sharding import PartitionSpec as P

GENES = 32768
BLOCK = 16
LANES = 128
GROUP = 8
HIGHS = GENES // (BLOCK * LANES)
WIDTH = 8
BASE = 60
PARTS = 3
PART = -(-LANES // PARTS)

target_sum = 10000.0
var_floor = 0.01
clip_value = 10.0

MESH = pl.DeviceIdType.MESH


def flip(value, k, size):
    out, bit = 0, 1
    while bit < size:
        part = lax.rem(lax.div(value, bit), 2)
        out = out + (1 - part if k & bit else part) * bit
        bit *= 2
    return out


def hub_grid(nx, ny, count):
    across = max(1, count // ny)
    along = count // across
    return across, along, nx // across, ny // along


def fused_kernel(
    sizes, cells, columns_hbm, counts_hbm, nnz_hbm, selected_hbm, stats_ref, pca_ref,
    columns_ref, counts_ref, nnz_ref, selected_ref, code_rows, high_rows, low_rows,
    near_values, near_offsets, far_codes, acc_values, acc_squares, table,
    mean_rows, spare_rows, sums_ref, sel_sums_ref, dense_ref, got, sel_got, mine, sel_mine, sel_stats_ref, moved_ref, turned,
    load_sem, send_sem, recv_sem,
):
    nx, ny, owners = sizes
    teams = nx * ny
    n = teams * owners
    gx, gy, z = lax.axis_index("gx"), lax.axis_index("gy"), lax.axis_index("gz")
    r = gx * ny + gy
    me = r * owners + z
    bf16, f32 = jnp.bfloat16, jnp.float32
    local, slots = columns_ref.shape
    groups = local // GROUP
    tiles = slots // LANES
    hubs = HIGHS // owners
    across, along, step_x, step_y = hub_grid(nx, ny, hubs)
    hub_x, hub_y = lax.div(gx, step_x), lax.div(gy, step_y)
    hub = hub_x * along + hub_y
    is_hub = (gx == hub_x * step_x + step_x - 1) & (gy == hub_y * step_y + step_y - 1)
    is_leaf = jnp.logical_not(is_hub)
    lines = 2 * BLOCK

    loads = [pltpu.make_async_copy(nnz_hbm, nnz_ref, load_sem.at[0])]
    for g in range(groups):
        span = pl.ds(g * GROUP, GROUP)
        loads.append(pltpu.make_async_copy(counts_hbm.at[span], counts_ref.at[span], load_sem.at[1 + 2 * g]))
        loads.append(pltpu.make_async_copy(columns_hbm.at[span], columns_ref.at[span], load_sem.at[2 + 2 * g]))
    loads.append(pltpu.make_async_copy(selected_hbm, selected_ref, load_sem.at[1 + 2 * groups]))
    for load in loads:
        load.start()

    xs = [flip(gx, k, nx) for k in range(nx)]
    ys = [flip(gy, k, ny) for k in range(ny)]
    zs = [flip(z, k, owners) for k in range(owners)]
    hub_xs = [flip(hub_x, k, across) for k in range(across)]
    hub_ys = [flip(hub_y, k, along) for k in range(along)]

    def greet(where):
        pl.semaphore_signal(barrier, inc=1, device_id=where, device_id_type=MESH)

    def each_hub(act, kys):
        for ky in kys:
            for kx in reversed(range(across)):
                for kz in reversed(range(owners)):
                    hx, hy = hub_xs[kx], hub_ys[ky]
                    slot = (hx * along + hy) * owners + zs[kz]
                    where = {"gx": hx * step_x + step_x - 1, "gy": hy * step_y + step_y - 1, "gz": zs[kz]}
                    if ky or kx or kz:
                        act(slot, where)
                    else:
                        pl.when(is_leaf)(functools.partial(act, slot, where))

    steps = list(reversed(range(along)))
    far_steps, near_steps = steps[:along // 2], steps[along // 2:]

    def each_team(act):
        for y in range(ny):
            for kx in sorted(range(nx), key=lambda k: (k & 1, k), reverse=True):
                if kx:
                    act({"gx": xs[kx], "gy": y, "gz": z})
                else:
                    pl.when(gy != y)(functools.partial(act, {"gx": gx, "gy": y, "gz": z}))

    barrier = pltpu.get_barrier_semaphore()
    if n <= 64:
        for ky in reversed(range(ny)):
            for kx in reversed(range(nx)):
                for kz in reversed(range(owners)):
                    if ky or kx or kz:
                        greet({"gx": xs[kx], "gy": ys[ky], "gz": zs[kz]})
    else:
        def greet_step(k, carry):
            other = lax.rem(me + k, n)
            team, owner = lax.div(other, owners), lax.rem(other, owners)
            greet({"gx": lax.div(team, ny), "gy": lax.rem(team, ny), "gz": owner})
            return carry

        lax.fori_loop(1, n, greet_step, 0)

    def send(src, dst, kind, where):
        pltpu.make_async_remote_copy(
            src_ref=src, dst_ref=dst, send_sem=send_sem.at[kind], recv_sem=recv_sem.at[kind],
            device_id=where, device_id_type=MESH,
        ).start()

    def finish(sem, ref, count):
        if count:
            span = ref.at[pl.ds(0, count)]
            pltpu.make_async_copy(span, span, sem).wait()

    ids = lax.broadcasted_iota(jnp.int32, (16, slots), 0).astype(f32).astype(bf16)
    sub = lax.broadcasted_iota(jnp.int32, (GROUP, local), 0)
    lane = lax.broadcasted_iota(jnp.int32, (GROUP, local), 1)
    slot = lax.broadcasted_iota(jnp.int32, (GROUP, slots), 1)

    def wait_group(g):
        loads[1 + 2 * g].wait()
        loads[2 + 2 * g].wait()

    def prepare(g):
        span = slice(g * GROUP, (g + 1) * GROUP)
        live_count = jnp.sum(jnp.where(sub + g * GROUP == lane, nnz_ref[...], 0), axis=1, keepdims=True)
        live = slot < live_count
        raw = jnp.where(live, counts_ref[span, :].astype(f32), 0.0)
        library = jnp.sum(raw, axis=1, keepdims=True)
        value = jnp.log(1.0 + raw * (target_sum / library))
        genes = columns_ref[span, :]
        shift = ((genes & (BLOCK - 1)) * WIDTH - BASE).astype(f32)
        code = value * jnp.exp2(shift)
        high = lax.shift_right_logical(genes, 11)
        low = lax.shift_right_logical(genes, 4) & (LANES - 1)
        for k in range(1, PARTS):
            past = low >= PART
            high = high + jnp.where(past, HIGHS, 0)
            low = low - jnp.where(past, PART, 0)
        high, low = high.astype(f32), low.astype(f32)
        for tile in range(tiles):
            at = (g * tiles + tile) * GROUP
            cols = slice(tile * LANES, (tile + 1) * LANES)
            for ref, line in ((code_rows, code), (high_rows, high), (low_rows, low)):
                ref[at:at + GROUP, :] = line[:, cols]

    def spread(ref, g, j):
        return jnp.concatenate(
            [ref[pl.ds((g * tiles + tile) * GROUP + j, 16, stride=0), :].astype(bf16) for tile in range(tiles)],
            axis=1,
        )

    def place(g, j):
        c = g * GROUP + j
        zero, one = bf16(0.0), bf16(1.0)
        high, code, low = spread(high_rows, g, j), spread(code_rows, g, j), spread(low_rows, g, j)
        left = jnp.concatenate(
            [jnp.where(high == ids + bf16(HIGHS * k), code, zero) for k in range(PARTS)], axis=0
        )
        right = jnp.concatenate(
            [jnp.where(low == ids + bf16(16 * k), one, zero) for k in range(-(-PART // 16))], axis=0
        )
        placed = lax.dot_general(left, right, (((1,), (1,)), ((), ())), preferred_element_type=f32)
        pieces = [
            placed[HIGHS * k:HIGHS * (k + 1), :min(PART, LANES - k * PART)] for k in range(PARTS)
        ]
        code = jnp.concatenate(pieces, axis=1)
        far_codes[pl.ds(c, HIGHS, stride=local), :] = code
        power = jnp.log2(jnp.maximum(code, 2.0 ** (-BASE - WIDTH)))
        offset = jnp.floor((power + (BASE + 0.5 * WIDTH)) * (1.0 / WIDTH))
        value = code * jnp.exp2(BASE - WIDTH * offset)
        near_values[c], near_offsets[c] = value, offset

    def gather_sums(g, ks):
        total = [jnp.zeros((HIGHS, LANES), f32) if g == 0 else acc_values[k] for k in ks]
        square = [jnp.zeros((HIGHS, LANES), f32) if g == 0 else acc_squares[k] for k in ks]
        for j in range(GROUP):
            c = g * GROUP + j
            v, o = near_values[c], near_offsets[c]
            for i, k in enumerate(ks):
                hit = jnp.where(o == float(k), v, 0.0)
                total[i] = total[i] + hit
                square[i] = square[i] + hit * hit
        for i, k in enumerate(ks):
            if g < groups - 1:
                acc_values[k], acc_squares[k] = total[i], square[i]
                continue
            near = total[i] * (1.0 / local)
            mean_rows[pl.ds(k, HIGHS, stride=BLOCK), :] = near
            spare_rows[pl.ds(k, HIGHS, stride=BLOCK), :] = square[i] - total[i] * near

    per_cell = BLOCK // GROUP
    loads[0].wait()
    wait_group(0)
    with jax.named_scope("prep"):
        prepare(0)
    for g in range(1, groups):
        wait_group(g)
    for g in range(groups):
        with jax.named_scope("place"):
            for j in range(GROUP):
                place(g, j)
                if g:
                    gather_sums(g - 1, range(j * per_cell, (j + 1) * per_cell))
                if j == 0 and g < groups - 1:
                    prepare(g + 1)
    with jax.named_scope("tail"):
        for j in range(GROUP):
            gather_sums(groups - 1, range(j * per_cell, (j + 1) * per_cell))
        for high in range(HIGHS):
            for stat, ref in enumerate((mean_rows, spare_rows)):
                line = ref[high * BLOCK:(high + 1) * BLOCK, :].astype(bf16)
                sums_ref[(high % hubs) * owners + high // hubs, stat * BLOCK:(stat + 1) * BLOCK, :] = line

    with jax.named_scope("barrier_wait"):
        pl.semaphore_wait(barrier, n - 1)
    with jax.named_scope("scatter_send"):
        each_hub(lambda slot, where: send(sums_ref.at[slot], got.at[me], 0, where), far_steps)
    got[me] = sums_ref[hub * owners + z]

    with jax.named_scope("select"):
        share = dense_ref.shape[2]
        out_tiles = share // LANES
        chunk = min(256, share)
        pairs = HIGHS // 2
        for pair in range(pairs):
            at = 2 * pair * local
            line = jnp.concatenate([far_codes[at:at + local, :], far_codes[at + local:at + 2 * local, :]], axis=1)
            table[pair * local:(pair + 1) * local, :] = line.astype(bf16)
        chunk_ids = lax.broadcasted_iota(jnp.int32, (16, chunk), 0).astype(f32).astype(bf16)
        loads[1 + 2 * groups].wait()
        for first in range(0, owners * share, chunk):
            picked = selected_ref[:, first:first + chunk]
            inside = (lax.shift_right_logical(picked, 4) & (2 * LANES - 1)).astype(f32)
            inside = jnp.broadcast_to(inside, (16, chunk)).astype(bf16)
            one_hot = jnp.concatenate(
                [jnp.where(inside == chunk_ids + bf16(16 * k), bf16(1.0), bf16(0.0)) for k in range(16)], axis=0
            )
            found = jnp.dot(table[...], one_hot, preferred_element_type=f32)
            which = jnp.broadcast_to(lax.shift_right_logical(picked, 12), (local, chunk))
            mix = found[:local]
            for pair in range(1, pairs):
                mix = jnp.where(which == pair, found[local * pair:local * (pair + 1)], mix)
            value = mix * jnp.exp2((BASE - (picked & (BLOCK - 1)) * WIDTH).astype(f32))
            x = jnp.where((value > 2.0 ** -4.5) & (value < 2.0 ** 3.5), value, 0.0)
            owner, start = first // share, first % share
            dense_ref[owner, :, start:start + chunk] = x.astype(bf16)
            total = jnp.sum(x, axis=0, keepdims=True)
            square = jnp.sum(x * x, axis=0, keepdims=True)
            pair = jnp.concatenate([total, square], axis=0)
            for tile in range(chunk // LANES):
                at = (start // LANES + tile) * owners + owner
                sel_sums_ref[at] = pair[:, tile * LANES:(tile + 1) * LANES]

    with jax.named_scope("sel_send"):
        each_hub(lambda slot, where: send(sel_sums_ref.at[slot], sel_got.at[me], 1, where), far_steps + near_steps)
        each_hub(lambda slot, where: send(sums_ref.at[slot], got.at[me], 0, where), near_steps)

        def move(k, carry):
            owner = lax.rem(z + k, owners)
            send(dense_ref.at[owner], moved_ref.at[z], 2, {"gx": gx, "gy": gy, "gz": owner})
            return carry

        lax.fori_loop(1, owners, move, 0)
        sel_got[me] = sel_sums_ref[hub * owners + z]
        moved_ref[z] = dense_ref[z]

    @pl.when(is_hub)
    def _():
        with jax.named_scope("wait_rs"):
            finish(recv_sem.at[0], got, n - 1)
        with jax.named_scope("reduce"):
            means = got[:, :BLOCK, :].astype(f32)
            mean = jnp.sum(means, axis=0) * (1.0 / n)
            away = means - mean[None]
            spare = got[:, BLOCK:, :].astype(f32)
            variance = jnp.sum(spare + (away * away) * float(local), axis=0) * (1.0 / cells)
            turned[:LANES, :] = jnp.transpose(mean)
            turned[LANES:, :] = jnp.transpose(variance)
            pieces = [turned[pl.ds(k, lines, stride=LANES // BLOCK), :] for k in range(LANES // BLOCK)]
            mine[...] = jnp.concatenate(pieces, axis=1).astype(bf16)
        with jax.named_scope("wait_selrs"):
            finish(recv_sem.at[1], sel_got, n - 1)
        with jax.named_scope("selreduce"):
            sel_mine[...] = jnp.sum(sel_got[...], axis=0)
            each_team(lambda where: send(sel_mine, sel_stats_ref.at[hub], 4, where))
            sel_stats_ref[hub] = sel_mine[...]
        with jax.named_scope("gather_send"):
            each_team(lambda where: send(mine, stats_ref.at[hub], 3, where))
            stats_ref[hub] = mine[...]

    with jax.named_scope("wait_moved"):
        finish(recv_sem.at[2], moved_ref, owners - 1)
        finish(send_sem.at[2], moved_ref, owners - 1)

    @pl.when(is_hub)
    def _():
        finish(send_sem.at[0], sums_ref, hubs * owners - 1)
        finish(send_sem.at[1], sel_sums_ref, hubs * owners - 1)
        finish(recv_sem.at[4], sel_stats_ref, hubs - 1)

    @pl.when(is_leaf)
    def _():
        finish(send_sem.at[0], sums_ref, hubs * owners)
        finish(send_sem.at[1], sel_sums_ref, hubs * owners)
        finish(recv_sem.at[4], sel_stats_ref, hubs)

    with jax.named_scope("pca"):
        for tile in range(out_tiles):
            mean = sel_stats_ref[tile, 0:1, :] * (1.0 / cells)
            variance = sel_stats_ref[tile, 1:2, :] * (1.0 / cells) - mean * mean
            scale = 1.0 / jnp.sqrt(jnp.maximum(variance, var_floor))
            cols = slice(tile * LANES, (tile + 1) * LANES)
            for owner in range(owners):
                x = moved_ref[owner, :, cols].astype(f32)
                y = jnp.clip((x - mean) * scale, -clip_value, clip_value)
                pca_ref[owner * local:(owner + 1) * local, cols] = y.astype(bf16)

    @pl.when(is_hub)
    def _():
        finish(recv_sem.at[3], stats_ref, hubs - 1)
        for _ in range(teams - 1):
            finish(send_sem.at[3], stats_ref, 1)
            finish(send_sem.at[4], sel_stats_ref, 1)

    @pl.when(is_leaf)
    def _():
        finish(recv_sem.at[3], stats_ref, hubs)


def final_kernel(stats_ref, pca_ref, gene_hbm, pca_hbm, gene_ref, sem):
    pca_copy = pltpu.make_async_copy(pca_ref, pca_hbm, sem.at[1])
    pca_copy.start()
    hubs, double, lanes = stats_ref.shape
    lines = double // 2
    stats = stats_ref[...].astype(jnp.float32)
    for hub in range(hubs):
        for stat in range(2):
            gene_ref[hub * lines:(hub + 1) * lines, stat, :] = stats[hub, stat * lines:(stat + 1) * lines]
    gene_copy = pltpu.make_async_copy(gene_ref, gene_hbm, sem.at[0])
    gene_copy.start()
    pca_copy.wait()
    gene_copy.wait()


def per_device(sizes, columns, counts, nnz_count, selected):
    f32, bf16, i32 = jnp.float32, jnp.bfloat16, jnp.int32
    nx, ny, owners = sizes
    teams = nx * ny
    n = teams * owners
    local, slots = columns.shape
    hubs = HIGHS // owners
    across, along, step_x, step_y = hub_grid(nx, ny, hubs)
    share = selected.shape[0] // owners
    assert hubs * owners == HIGHS and across * along == hubs and across * step_x == nx and along * step_y == ny
    assert share == hubs * LANES and local % GROUP == 0
    hbm = pl.BlockSpec(memory_space=pltpu.HBM)
    vmem = pl.BlockSpec(memory_space=pltpu.VMEM)
    slot_rows = local * slots // LANES + 16
    far_rows = HIGHS * local
    arrays = (columns, counts, nnz_count.reshape(1, local), selected.reshape(1, -1))
    kept = pl.pallas_call(
        functools.partial(fused_kernel, sizes, local * n),
        name="moments_and_selection",
        out_shape=(
            pltpu.VMEM((hubs, 2 * BLOCK, LANES), bf16),
            pltpu.VMEM((owners * local, share), bf16),
        ),
        in_specs=[hbm] * 4,
        out_specs=(vmem,) * 2,
        scratch_shapes=[
            pltpu.VMEM((local, slots), i32),
            pltpu.VMEM((local, slots), i32),
            pltpu.VMEM((1, local), i32),
            pltpu.VMEM((1, owners * share), i32),
        ]
        + [pltpu.VMEM((slot_rows, LANES), f32)] * 3
        + [pltpu.VMEM((local, HIGHS, LANES), f32)] * 2
        + [pltpu.VMEM((far_rows, LANES), f32)]
        + [pltpu.VMEM((BLOCK, HIGHS, LANES), f32)] * 2
        + [pltpu.VMEM((far_rows // 2, 2 * LANES), bf16)]
        + [pltpu.VMEM((HIGHS * BLOCK, LANES), f32)] * 2
        + [
            pltpu.VMEM((HIGHS, 2 * BLOCK, LANES), bf16),
            pltpu.VMEM((HIGHS, 2, LANES), f32),
            pltpu.VMEM((owners, local, share), bf16),
            pltpu.VMEM((n, 2 * BLOCK, LANES), bf16),
            pltpu.VMEM((n, 2, LANES), f32),
            pltpu.VMEM((2 * BLOCK, LANES), bf16),
            pltpu.VMEM((2, LANES), f32),
            pltpu.VMEM((hubs, 2, LANES), f32),
            pltpu.VMEM((owners, local, share), bf16),
            pltpu.VMEM((2 * LANES, BLOCK), f32),
            pltpu.SemaphoreType.DMA((2 + 2 * (local // GROUP),)),
            pltpu.SemaphoreType.DMA((5,)),
            pltpu.SemaphoreType.DMA((5,)),
        ],
        compiler_params=pltpu.CompilerParams(
            collective_id=0, has_side_effects=True, vmem_limit_bytes=32 * 1024 * 1024
        ),
    )(*(pltpu.with_memory_space_constraint(array, pltpu.HBM) for array in arrays))
    out_lines = GENES // owners // LANES
    gene_stats, pca_input = pl.pallas_call(
        final_kernel,
        name="standardize",
        out_shape=(pltpu.HBM((out_lines, 2, LANES), f32), pltpu.HBM((owners * local, share), bf16)),
        in_specs=[vmem] * 2,
        out_specs=(hbm,) * 2,
        scratch_shapes=[
            pltpu.VMEM((out_lines, 2, LANES), f32),
            pltpu.SemaphoreType.DMA((2,)),
        ],
        compiler_params=pltpu.CompilerParams(vmem_limit_bytes=16 * 1024 * 1024),
    )(*(pltpu.with_memory_space_constraint(array, pltpu.VMEM) for array in kept))
    return (gene_stats.transpose(1, 0, 2).reshape(2, -1), pca_input)


def solution(mesh):
    sizes = tuple(mesh.shape[axis] for axis in ("gx", "gy", "gz"))
    return jax.shard_map(
        functools.partial(per_device, sizes),
        mesh=mesh,
        in_specs=(
            P(("gx", "gy", "gz"), None),
            P(("gx", "gy", "gz"), None),
            P(("gx", "gy", "gz")),
            P(),
        ),
        out_specs=(P(None, "gz"), P(("gx", "gy"), "gz")),
        check_vma=False,
    )
```
